16 devices in a mesh: dp: 4 (over z, y), ep: 4 (over x, core).
Axes of the slice: x: 2, y: 2, z: 2, core: 2. Of those that a mesh axis runs over, the one named last changes fastest.
Arguments:
- w_gate: bfloat16 [1, 8, 4096, 1536], P(None, 'ep')
- w_up: bfloat16 [1, 8, 4096, 1536], P(None, 'ep')
- w_down: bfloat16 [1, 8, 1536, 4096], P(None, 'ep')
- place: int32 [1, 32], replicated
Outputs:
- output 1: bfloat16 [1, 32, 4096, 3072], P(None, ('dp', 'ep'))
- output 2: bfloat16 [1, 32, 1536, 4096], P(None, ('dp', 'ep'))
All inputs are finite; a program needn't handle non-finite values.
Results may differ from the reference program's by a relative error of at most 0.001.
Values are sent between devices in bfloat16 or wider.
A program may use at most 1 GiB of HBM per device.

```python
import jax
import jax.numpy as jnp
import numpy as np

D = 4096
F = 1536
E = 8
L = 1
SLOTS = 2
DP = 4
EP = 4


def _slot_shard():
    n = np.arange(DP * EP)[:, None]
    j = np.arange(SLOTS)[None, :]
    a, g = n // EP, n % EP
    h = np.where(j < ((a + 1) * SLOTS) // DP, (2 * a - g) % EP, (g + j + 1) % EP)
    return h.reshape(-1)


def _draw_place(key):
    shard = E // EP
    width = DP * SLOTS

    def one(k):
        k1, k2, k3 = jax.random.split(k, 3)
        base = jax.random.permutation(k1, shard)
        extra = jax.random.randint(k2, (width - shard,), 0, shard)
        return jax.random.permutation(k3, jnp.concatenate([base, extra]))

    local = jax.vmap(one)(jax.random.split(key, L * EP)).reshape(L, EP, width)
    glob = (local + (jnp.arange(EP) * shard)[None, :, None]).reshape(L, EP * width)
    order = np.argsort(_slot_shard(), kind="stable")
    out = jnp.zeros((L, EP * width), jnp.int32).at[:, order].set(glob.astype(jnp.int32))
    return out


def setup_inputs(seed: int = 0) -> dict:
    kg, ku, kd, kp = jax.random.split(jax.random.PRNGKey(seed), 4)
    w_gate = jax.random.normal(kg, (L, E, D, F), jnp.float32).astype(jnp.bfloat16)
    w_up = jax.random.normal(ku, (L, E, D, F), jnp.float32).astype(jnp.bfloat16)
    w_down = jax.random.normal(kd, (L, E, F, D), jnp.float32).astype(jnp.bfloat16)
    return {"w_gate": w_gate, "w_up": w_up, "w_down": w_down, "place": _draw_place(kp)}


def reference(w_gate, w_up, w_down, place):
    take = jax.vmap(lambda w, i: w[i])
    w13 = jnp.concatenate([take(w_gate, place), take(w_up, place)], axis=-1)
    return w13, take(w_down, place)
```

```python
import functools

import jax
import jax.numpy as jnp
from jax import lax
from jax.experimental import pallas as pl
from jax.experimental.pallas import tpu as pltpu
from jax.sharding import PartitionSpec as P

N = 64
NI = 4
NO = 8
LAG = 6
BUF_P, BUF_Q, BUF_R, BUF_S = range(4)
VMEM_LIMIT = 60 * 1024 * 1024


def _slot_of(place, a, g, j):
    return place[0, (a * 4 + g) * 2 + j] % 2


def _move(place, wg, wu, wd, sgu, sd, ig, og, idn, odn, ig2, og2, idn2, odn2, in_sem, out_sem, in2_sem, out2_sem, fwd_sem, recv_sem):
    total = 3 * N
    a = lax.axis_index("dp")
    g = lax.axis_index("ep")
    x, c = g // 2, g % 2
    rg, rd = wg.shape[2] // N, wd.shape[2] // N

    def dev(a2, c2, flip=False):
        return (a2, 2 * ((1 - x) if flip else x) + c2)

    def local(m, e, k):
        return wd.at[0, e, pl.ds(k * rd, rd)] if m == 2 else (wg, wu)[m].at[0, e, pl.ds(k * rg, rg)]

    def stage(m, b, k):
        return sd.at[b, pl.ds(k * rd, rd)] if m == 2 else sgu.at[b, m, pl.ds(k * rg, rg)]

    def stage_all(m, b):
        return sd.at[b] if m == 2 else sgu.at[b, m]

    def each(q, fn):
        for m in range(3):
            @pl.when((q >= m * N) & (q < (m + 1) * N))
            def _():
                fn(m, q - m * N)

    def remote(src, dst, ssem, rsem, device):
        return pltpu.make_async_remote_copy(src_ref=src, dst_ref=dst, send_sem=ssem, recv_sem=rsem, device_id=device,
                                            device_id_type=pl.DeviceIdType.MESH)

    here = (a, g)

    def wait_recv(b, q):
        each(q, lambda m, k: remote(stage(m, b, k), stage(m, b, k), fwd_sem.at[0, 0], recv_sem.at[b, q], dev(a, 1 - c)).wait_recv())

    def wait_all(b):
        def step(q, _):
            wait_recv(b, q)
            return 0
        lax.fori_loop(0, total, step, 0)

    def forward(q, b, flow, device):
        each(q, lambda m, k: remote(stage(m, b, k), stage(m, b, k), fwd_sem.at[flow, m], recv_sem.at[b, q], device).start())

    def wait_sent(flow, b, device):
        for m in range(3):
            remote(stage_all(m, b), stage_all(m, b), fwd_sem.at[flow, m], recv_sem.at[b, 0], device).wait_send()

    def pick_start(q, ins, sem, src0, src1):
        def go(m, k):
            buf = ins[m // 2].at[q % NI]
            pltpu.make_async_copy(src0(m, k), buf.at[0], sem.at[q % NI, 0]).start()
            pltpu.make_async_copy(src1(m, k), buf.at[1], sem.at[q % NI, 1]).start()
        each(q, go)

    def pick_run(q, ins, outs, sem, osem, src0, src1, which, b, device):
        def free(m, k):
            remote(outs[m // 2].at[q % NO], stage(m, b, k), osem.at[q % NO], recv_sem.at[b, 0], device).wait_send()
        each(jnp.where(q < total, q - NO, -1), free)

        def go(m, k):
            i, o = ins[m // 2], outs[m // 2]
            slot, oslot = q % NI, q % NO
            pltpu.make_async_copy(src0(m, k), i.at[slot, 0], sem.at[slot, 0]).wait()
            pltpu.make_async_copy(src1(m, k), i.at[slot, 1], sem.at[slot, 1]).wait()
            rows = 8 if m == 2 else 16

            def some(r, _):
                at = pl.ds(r * rows, rows)
                o[oslot, at] = jnp.where(which == 0, i[slot, 0, at], i[slot, 1, at])
                return 0
            lax.fori_loop(0, (rd if m == 2 else rg) // rows, some, 0)
        each(q, go)

    def pick_send(q, outs, osem, b, device):
        each(q, lambda m, k: remote(outs[m // 2].at[q % NO], stage(m, b, k), osem.at[q % NO], recv_sem.at[b, q], device).start())

    def pick_drain(outs, osem, b, device):
        def step(q, _):
            each(q, lambda m, k: remote(outs[m // 2].at[q % NO], stage(m, b, k), osem.at[q % NO], recv_sem.at[b, 0], device).wait_send())
            return 0
        lax.fori_loop(total - NO, total, step, 0)

    is_src = (c == 0) & (a < 2) | (c == 1) & (a >= 2)

    @pl.when(is_src)
    def _():
        other = 2 * (1 - x)
        a2 = _slot_of(place, 2, other, 1)
        b1 = _slot_of(place, 1, other + 1, 1)
        which = jnp.where(c == 0, a2, b1)
        which = jnp.where((a == 1) | (a == 2), 1 - which, which)
        b = a % 2
        mirror = (a, 2 * (1 - x) + c)
        src = (lambda m, k: local(m, 0, k)), (lambda m, k: local(m, 1, k))
        ins, outs = (ig, idn), (og, odn)
        b0 = _slot_of(place, 0, 2 * x + 1, 1) == _slot_of(place, 1, 2 * x + 1, 1)
        which2 = jnp.where(b0, 1, 0)
        src2 = (lambda m, k: stage(m, BUF_P, k)), (lambda m, k: stage(m, BUF_Q, k))
        ins2, outs2 = (ig2, idn2), (og2, odn2)
        to0 = dev(0, 1)

        def tick(t, _):
            pick_start(t, ins, in_sem, *src)
            pick_send(t - 3, outs, out_sem, b, mirror)
            pick_run(t - 2, ins, outs, in_sem, out_sem, *src, which, b, mirror)
            u = t - 3 - LAG
            wait_recv(b, u)

            @pl.when(a == 0)
            def _():
                forward(u, BUF_P, 0, dev(1, 0))
                forward(u, BUF_P, 1, dev(2, 0))
                forward(u, BUF_P, 2, dev(0, 1))

            @pl.when(a == 1)
            def _():
                forward(u, BUF_Q, 0, dev(0, 1))
                forward(u, BUF_Q, 1, dev(3, 0))

            @pl.when(a == 3)
            def _():
                forward(u, BUF_Q, 0, dev(2, 1))
                forward(u, BUF_Q, 1, dev(1, 1))

            @pl.when(a == 2)
            def _():
                wait_recv(BUF_Q, u)
                pick_start(u, ins2, in2_sem, *src2)
                pick_send(u - 3, outs2, out2_sem, BUF_R, to0)
                pick_run(u - 2, ins2, outs2, in2_sem, out2_sem, *src2, which2, BUF_R, to0)
            return 0
        lax.fori_loop(0, total + 3 + LAG + 3, tick, 0)
        pick_drain(outs, out_sem, b, mirror)

        @pl.when(a == 0)
        def _():
            wait_all(BUF_Q)
            wait_all(BUF_R)
            wait_all(BUF_S)
            wait_sent(0, BUF_P, dev(1, 0))
            wait_sent(1, BUF_P, dev(2, 0))
            wait_sent(2, BUF_P, dev(0, 1))

        @pl.when(a == 1)
        def _():
            wait_all(BUF_P)
            wait_sent(0, BUF_Q, dev(0, 1))
            wait_sent(1, BUF_Q, dev(3, 0))

        @pl.when(a == 3)
        def _():
            wait_sent(0, BUF_Q, dev(2, 1))
            wait_sent(1, BUF_Q, dev(1, 1))

        @pl.when(a == 2)
        def _():
            pick_drain(outs2, out2_sem, BUF_R, to0)

    @pl.when((a == 0) & (c == 1))
    def _():
        peer = dev(0, 0)

        def tick(q, _):
            def give(m, k):
                for e in range(2):
                    remote(local(m, e, k), stage(m, BUF_R + e, k), fwd_sem.at[1 + e, m], recv_sem.at[BUF_R + e, q], peer).start()
            each(q, give)
            wait_recv(BUF_Q, q)
            forward(q, BUF_Q, 0, peer)
            return 0
        lax.fori_loop(0, total, tick, 0)
        wait_all(BUF_P)
        wait_all(BUF_R)
        for flow, b in enumerate((BUF_Q, BUF_R, BUF_S)):
            wait_sent(flow, b, peer)

    @pl.when((a == 1) & (c == 1))
    def _():
        wait_all(BUF_Q)

    @pl.when((a == 2) & (c == 0))
    def _():
        def tick(q, _):
            wait_recv(BUF_P, q)
            forward(q, BUF_P, 0, dev(3, 0))
            return 0
        lax.fori_loop(0, total, tick, 0)
        wait_sent(0, BUF_P, dev(3, 0))

    @pl.when((a == 3) & (c == 0))
    def _():
        wait_all(BUF_P)
        wait_all(BUF_Q)


NP = 16
NB = 12
AHEAD = 6


def _place(place, wg, wu, wd, sgu, sd, w13, w2, bg, bd, in_sem, out_sem):
    a = lax.axis_index("dp")
    g = lax.axis_index("ep")
    x, c = g // 2, g % 2
    f = wg.shape[3]
    rg, rd = wg.shape[2] // NP, wd.shape[2] // NP

    a2 = _slot_of(place, 2, 2 * x, 1)
    b1 = _slot_of(place, 1, 2 * x + 1, 1)

    def source(j):
        e = _slot_of(place, a, g, j)
        far_a = jnp.where(e == a2, 2 + BUF_P, 2 + BUF_Q)
        far_b = jnp.where(e == b1, 2 + BUF_Q, 2 + BUF_P)
        if j == 0:
            c0 = jnp.where(a == 0, 2 + BUF_R + e, jnp.where(a == 2, e, far_a))
            c1 = jnp.where(a == 0, far_a, jnp.where(a == 2, far_b, e))
        else:
            c0 = far_a
            c1 = jnp.where(a == 0, 2 + BUF_R, jnp.where(a == 3, e, far_b))
        return jnp.where(c == 0, c0, c1)

    sources = [source(0), source(1)]

    def run(first, bufs, fetch, put):
        def tick(t, _):
            @pl.when(t < first)
            def _():
                slot = t % NB

                @pl.when(t >= NB)
                def _():
                    put(t - NB, slot, True)
                fetch(t, slot)
            u = t - AHEAD

            @pl.when(u >= 0)
            def _():
                slot = u % NB
                pltpu.make_async_copy(bufs.at[slot], bufs.at[slot], in_sem.at[slot]).wait()
                put(u, slot, False)
            return 0
        lax.fori_loop(0, first + AHEAD, tick, 0)

        def drain(t, _):
            put(t, t % NB, True)
            return 0
        lax.fori_loop(first - NB, first, drain, 0)

    def fetch_gu(t, slot):
        m, j, k = t // (2 * NP), (t // NP) % 2, t % NP
        s = jnp.where(j == 0, sources[0], sources[1])
        rows = pl.ds(k * rg, rg)
        for mm, w in enumerate((wg, wu)):
            @pl.when((s < 2) & (m == mm))
            def _():
                pltpu.make_async_copy(w.at[0, s, rows], bg.at[slot], in_sem.at[slot]).start()

        @pl.when(s >= 2)
        def _():
            pltpu.make_async_copy(sgu.at[s - 2, m, rows], bg.at[slot], in_sem.at[slot]).start()

    def put_gu(t, slot, wait):
        m, j, k = t // (2 * NP), (t // NP) % 2, t % NP
        for mm in range(2):
            @pl.when(m == mm)
            def _():
                cp = pltpu.make_async_copy(bg.at[slot], w13.at[0, j, pl.ds(k * rg, rg), pl.ds(mm * f, f)], out_sem.at[slot])
                cp.wait() if wait else cp.start()

    def fetch_d(t, slot):
        j, k = t // NP, t % NP
        s = jnp.where(j == 0, sources[0], sources[1])
        rows = pl.ds(k * rd, rd)

        @pl.when(s < 2)
        def _():
            pltpu.make_async_copy(wd.at[0, s, rows], bd.at[slot], in_sem.at[slot]).start()

        @pl.when(s >= 2)
        def _():
            pltpu.make_async_copy(sd.at[s - 2, rows], bd.at[slot], in_sem.at[slot]).start()

    def put_d(t, slot, wait):
        j, k = t // NP, t % NP
        cp = pltpu.make_async_copy(bd.at[slot], w2.at[0, j, pl.ds(k * rd, rd)], out_sem.at[slot])
        cp.wait() if wait else cp.start()

    run(4 * NP, bg, fetch_gu, put_gu)
    run(2 * NP, bd, fetch_d, put_d)


def solution(mesh):
    def body(w_gate, w_up, w_down, place):
        d, f = w_gate.shape[2], w_gate.shape[3]
        bf16 = w_gate.dtype
        hbm = pl.BlockSpec(memory_space=pl.ANY)
        smem = pl.BlockSpec(memory_space=pltpu.SMEM)
        rg, rd = d // N, f // N
        rings = [pltpu.VMEM((NI, 2, rg, f), bf16), pltpu.VMEM((NO, rg, f), bf16),
                 pltpu.VMEM((NI, 2, rd, d), bf16), pltpu.VMEM((NO, rd, d), bf16)]
        dma = pltpu.SemaphoreType.DMA
        sgu, sd = pl.pallas_call(
            _move,
            out_shape=(jax.ShapeDtypeStruct((4, 2, d, f), bf16), jax.ShapeDtypeStruct((4, f, d), bf16)),
            in_specs=[smem, hbm, hbm, hbm],
            out_specs=(hbm, hbm),
            scratch_shapes=rings + rings + [dma((NI, 2)), dma((NO,)), dma((NI, 2)), dma((NO,)), dma((3, 3)), dma((4, 3 * N))],
            compiler_params=pltpu.CompilerParams(has_side_effects=True, vmem_limit_bytes=VMEM_LIMIT),
            name="move",
        )(place, w_gate, w_up, w_down)
        return pl.pallas_call(
            _place,
            out_shape=(jax.ShapeDtypeStruct((1, 2, d, 2 * f), bf16), jax.ShapeDtypeStruct((1, 2, f, d), bf16)),
            in_specs=[smem] + [hbm] * 5,
            out_specs=(hbm, hbm),
            scratch_shapes=[pltpu.VMEM((NB, d // NP, f), bf16), pltpu.VMEM((NB, f // NP, d), bf16), dma((NB,)), dma((NB,))],
            compiler_params=pltpu.CompilerParams(vmem_limit_bytes=VMEM_LIMIT),
            name="place",
        )(place, w_gate, w_up, w_down, sgu, sd)

    spec_in = P(None, "ep", None, None)
    spec_out = P(None, ("dp", "ep"), None, None)
    return jax.shard_map(body, mesh=mesh,
                         in_specs=(spec_in, spec_in, spec_in, P(None, None)),
                         out_specs=(spec_out, spec_out), check_vma=False)
```

```python
import functools

import jax
import jax.numpy as jnp
from jax import lax
from jax.experimental import pallas as pl
from jax.experimental.pallas import tpu as pltpu
from jax.sharding import PartitionSpec as P

NG = 64
ND = 64
NI = 3
NO = 4
NI2 = 2
NV = 2
LAG = 4
LATE = 6
KEEP = 52
BUF_P, BUF_Q, BUF_R, BUF_S = range(4)
MOVE_VMEM = 11 * 1024 * 1024
PLACE_VMEM = 8 * 1024 * 1024


def _slot_of(place, a, g, j):
    return place[0, (a * 4 + g) * 2 + j] % 2


def _move(place, wg, wu, wd, sgu, sd, kup, kdn, ig, og, idn, odn, ig2, og2, idn2, odn2, vg, vd,
          in_sem, out_sem, in2_sem, out2_sem, v_sem, fwd_sem, recv_sem):
    total = 2 * NG + ND
    first = (0, NG, 2 * NG, total)
    a = lax.axis_index("dp")
    g = lax.axis_index("ep")
    x, c = g // 2, g % 2
    rg, rd = wg.shape[2] // NG, wd.shape[2] // ND

    def dev(a2, c2, flip=False):
        return (a2, 2 * ((1 - x) if flip else x) + c2)

    def local(m, e, k):
        return wd.at[0, e, pl.ds(k * rd, rd)] if m == 2 else (wg, wu)[m].at[0, e, pl.ds(k * rg, rg)]

    def stage(m, b, k):
        return sd.at[b, pl.ds(k * rd, rd)] if m == 2 else sgu.at[b, m, pl.ds(k * rg, rg)]

    def stage_all(m, b):
        return sd.at[b] if m == 2 else sgu.at[b, m]

    def each(q, fn):
        for m in range(3):
            @pl.when((q >= first[m]) & (q < first[m + 1]))
            def _():
                fn(m, q - first[m])

    def remote(src, dst, ssem, rsem, device):
        return pltpu.make_async_remote_copy(src_ref=src, dst_ref=dst, send_sem=ssem, recv_sem=rsem, device_id=device,
                                            device_id_type=pl.DeviceIdType.MESH)

    def wait_recv(b, q):
        each(q, lambda m, k: remote(stage(m, b, k), stage(m, b, k), fwd_sem.at[0, 0], recv_sem.at[b, q], dev(a, 1 - c)).wait_recv())

    def forward(q, b, flow, device):
        each(q, lambda m, k: remote(stage(m, b, k), stage(m, b, k), fwd_sem.at[flow, m], recv_sem.at[b, q], device).start())

    def wait_sent(flow, b, device):
        for m in range(3):
            remote(stage_all(m, b), stage_all(m, b), fwd_sem.at[flow, m], recv_sem.at[b, 0], device).wait_send()

    def pick_start(q, ins, sem, src0, src1):
        def go(m, k):
            buf = ins[m // 2].at[q % ins[0].shape[0]]
            pltpu.make_async_copy(src0(m, k), buf.at[0], sem.at[q % ins[0].shape[0], 0]).start()
            pltpu.make_async_copy(src1(m, k), buf.at[1], sem.at[q % ins[0].shape[0], 1]).start()
        each(q, go)

    def pick_run(q, ins, outs, sem, osem, src0, src1, which, b, device):
        def free(m, k):
            remote(outs[m // 2].at[q % NO], stage(m, b, k), osem.at[q % NO], recv_sem.at[b, 0], device).wait_send()
        each(jnp.where(q < total, q - NO, -1), free)

        def go(m, k):
            i, o = ins[m // 2], outs[m // 2]
            slot, oslot = q % i.shape[0], q % NO
            pltpu.make_async_copy(src0(m, k), i.at[slot, 0], sem.at[slot, 0]).wait()
            pltpu.make_async_copy(src1(m, k), i.at[slot, 1], sem.at[slot, 1]).wait()
            rows = 8 if m == 2 else 16

            def some(r, _):
                at = pl.ds(r * rows, rows)
                o[oslot, at] = jnp.where(which == 0, i[slot, 0, at], i[slot, 1, at])
                return 0
            lax.fori_loop(0, (rd if m == 2 else rg) // rows, some, 0)
        each(q, go)

    def pick_send(q, outs, osem, b, device):
        each(q, lambda m, k: remote(outs[m // 2].at[q % NO], stage(m, b, k), osem.at[q % NO], recv_sem.at[b, q], device).start())

    def pick_drain(outs, osem, b, device):
        def step(q, _):
            each(q, lambda m, k: remote(outs[m // 2].at[q % NO], stage(m, b, k), osem.at[q % NO], recv_sem.at[b, 0], device).wait_send())
            return 0
        lax.fori_loop(total - NO, total, step, 0)

    def greet(*partners):
        barrier = pltpu.get_barrier_semaphore()
        for device in partners:
            pl.semaphore_signal(barrier, inc=1, device_id=device, device_id_type=pl.DeviceIdType.MESH)
        pl.semaphore_wait(barrier, len(partners))

    mirror = (a, 2 * (1 - x) + c)
    for a2, c2, partners in (
        (0, 0, (mirror, dev(1, 0), dev(2, 0), dev(0, 1))),
        (0, 1, (dev(0, 0), dev(1, 0), dev(2, 1))),
        (1, 0, (mirror, dev(0, 0), dev(0, 1), dev(3, 0))),
        (1, 1, (dev(3, 1),)),
        (2, 0, (dev(0, 0), dev(3, 0))),
        (2, 1, (mirror, dev(3, 1), dev(0, 1))),
        (3, 0, (dev(1, 0), dev(2, 0))),
        (3, 1, (mirror, dev(2, 1), dev(1, 1))),
    ):
        pl.when((a == a2) & (c == c2))(functools.partial(greet, *partners))

    is_src = (c == 0) & (a < 2) | (c == 1) & (a >= 2)
    here = lambda a2, c2: (a == a2) & (c == c2)
    other = 2 * (1 - x)
    which = jnp.where(c == 0, _slot_of(place, 2, other, 1), _slot_of(place, 1, other + 1, 1))
    which = jnp.where((a == 1) | (a == 2), 1 - which, which)
    b = a % 2
    src = (lambda m, k: local(m, 0, k)), (lambda m, k: local(m, 1, k))
    ins, outs = (ig, idn), (og, odn)
    far_a, far_b = _slot_of(place, 2, 2 * x, 1), _slot_of(place, 1, 2 * x + 1, 1)
    which2 = jnp.where(_slot_of(place, 0, 2 * x + 1, 1) == far_b, 1, 0)
    src2 = (lambda m, k: stage(m, BUF_P, k)), (lambda m, k: stage(m, BUF_Q, k))
    ins2, outs2 = (ig2, idn2), (og2, odn2)
    to0 = dev(0, 1)
    flows = {
        (0, 0): (BUF_P, (dev(1, 0), dev(2, 0), dev(0, 1))),
        (0, 1): (BUF_Q, (dev(0, 0),)),
        (1, 0): (BUF_Q, (dev(0, 1), dev(3, 0))),
        (2, 0): (BUF_P, (dev(3, 0),)),
        (3, 1): (BUF_Q, (dev(2, 1), dev(1, 1))),
    }
    late = {(0, 0): (BUF_Q, BUF_R, BUF_S), (0, 1): (BUF_P, BUF_R), (1, 0): (BUF_P,), (1, 1): (BUF_Q,), (3, 0): (BUF_P, BUF_Q)}

    own = (here(1, 1) | here(2, 0) | here(3, 1), here(3, 1))
    pairs = ((jnp.where(here(0, 0), BUF_R, BUF_P), jnp.where(here(0, 0), BUF_S, BUF_Q)),
             (jnp.where(here(0, 1), BUF_R, jnp.where(here(1, 1), BUF_Q, BUF_P)),
              jnp.where(here(0, 1), BUF_R, jnp.where(here(2, 0), BUF_P, BUF_Q))))
    kept = []
    for j in range(2):
        e = _slot_of(place, a, g, j)
        from_a = (c == 0) | (here(0, 1) if j == 0 else False)
        far = jnp.where(from_a, jnp.where(e == far_a, 0, 1), jnp.where(e == far_b, 1, 0))
        kept.append(jnp.where(own[j] | (here(0, 0) if j == 0 else False), e, far))
    first_kept = 2 * NG - KEEP

    def keep_start(q):
        def go(m, k):
            for j in range(2):
                for e in range(2):
                    to, sem = (vg, vd)[m // 2].at[q % NV, j, e], v_sem.at[q % NV, j, e]

                    @pl.when(own[j])
                    def _():
                        pltpu.make_async_copy(local(m, e, k), to, sem).start()

                    @pl.when(jnp.logical_not(own[j]))
                    def _():
                        pltpu.make_async_copy(stage(m, pairs[j][e], k), to, sem).start()
        each(jnp.where(q < first_kept, -1, q), go)

    def keep_run(q):
        def go(m, k):
            v, o = ((vg, kup), (vd, kdn))[m // 2]
            n, rows = (rd, 8) if m == 2 else (rg, 16)
            base = k * rd if m == 2 else (k - (NG - KEEP)) * rg
            for j in range(2):
                for e in range(2):
                    pltpu.make_async_copy(local(m, e, k), v.at[q % NV, j, e], v_sem.at[q % NV, j, e]).wait()

                def some(r, _):
                    at = pl.ds(pl.multiple_of(r * rows, rows), rows)
                    o[j, pl.ds(pl.multiple_of(base + r * rows, rows), rows)] = jnp.where(kept[j] == 0, v[q % NV, j, 0, at], v[q % NV, j, 1, at])
                    return 0
                lax.fori_loop(0, n // rows, some, 0)
        each(jnp.where(q < first_kept, -1, q), go)

    def tick(t, _):
        u = t - 3 - LAG

        @pl.when(is_src)
        def _():
            pick_start(t, ins, in_sem, *src)
            pick_send(t - 3, outs, out_sem, b, mirror)
            pick_run(t - 2, ins, outs, in_sem, out_sem, *src, which, b, mirror)

        @pl.when(here(2, 1))
        def _():
            pick_send(u - 1, outs2, out2_sem, BUF_R, to0)
            wait_recv(BUF_P, u)
            wait_recv(BUF_Q, u)
            pick_start(u, ins2, in2_sem, *src2)
            pick_run(u, ins2, outs2, in2_sem, out2_sem, *src2, which2, BUF_R, to0)

        @pl.when(here(0, 1))
        def _():
            def give(m, k):
                for e in range(2):
                    remote(local(m, e, k), stage(m, BUF_R + e, k), fwd_sem.at[1 + e, m], recv_sem.at[BUF_R + e, t], dev(0, 0)).start()
            each(t, give)

        for (a2, c2), (block, devices) in flows.items():
            @pl.when(here(a2, c2))
            def _():
                wait_recv(block, u)
                for flow, device in enumerate(devices):
                    forward(u, block, flow, device)

        v = u - LATE
        for (a2, c2), blocks in late.items():
            @pl.when(here(a2, c2))
            def _():
                for block in blocks:
                    wait_recv(block, v)
        keep_start(v)
        keep_run(v - 1)
        return 0
    lax.fori_loop(0, total + 3 + LAG + LATE + 1, tick, 0)

    @pl.when(is_src)
    def _():
        pick_drain(outs, out_sem, b, mirror)

    @pl.when(here(2, 1))
    def _():
        pick_drain(outs2, out2_sem, BUF_R, to0)

    for (a2, c2), (block, devices) in flows.items():
        @pl.when(here(a2, c2))
        def _():
            for flow, device in enumerate(devices):
                wait_sent(flow, block, device)

    @pl.when(here(0, 1))
    def _():
        wait_sent(1, BUF_R, dev(0, 0))
        wait_sent(2, BUF_S, dev(0, 0))


NP = 32
NB = 14
AHEAD = 7
PARTS = 4


def _place(place, wg, wu, sgu, kup, kdn, w13, w2, bg, in_sem, out_sem, k_sem):
    a = lax.axis_index("dp")
    g = lax.axis_index("ep")
    x, c = g // 2, g % 2
    d, f = wg.shape[2], wg.shape[3]
    rows = d // NP
    nup = (d - kup.shape[1]) // rows
    total = 2 * (NP + nup)

    a2 = _slot_of(place, 2, 2 * x, 1)
    b1 = _slot_of(place, 1, 2 * x + 1, 1)

    def source(j):
        e = _slot_of(place, a, g, j)
        far_a = jnp.where(e == a2, 2 + BUF_P, 2 + BUF_Q)
        far_b = jnp.where(e == b1, 2 + BUF_Q, 2 + BUF_P)
        if j == 0:
            c0 = jnp.where(a == 0, 2 + BUF_R + e, jnp.where(a == 2, e, far_a))
            c1 = jnp.where(a == 0, far_a, jnp.where(a == 2, far_b, e))
        else:
            c0 = far_a
            c1 = jnp.where(a == 0, 2 + BUF_R, jnp.where(a == 3, e, jnp.where(a == 1, 2 + BUF_Q, far_b)))
        return jnp.where(c == 0, c0, c1)

    sources = [source(0), source(1)]

    def where(t):
        m = (t >= 2 * NP).astype(jnp.int32)
        r = t - m * 2 * NP
        n = jnp.where(m == 0, NP, nup)
        return m, r // n, r % n

    def fetch(t):
        slot = t % NB
        m, j, k = where(t)
        s = jnp.where(j == 0, sources[0], sources[1])
        at = pl.ds(k * rows, rows)
        for mm, w in enumerate((wg, wu)):
            @pl.when((s < 2) & (m == mm))
            def _():
                pltpu.make_async_copy(w.at[0, s, at], bg.at[slot], in_sem.at[slot]).start()

        @pl.when(s >= 2)
        def _():
            pltpu.make_async_copy(sgu.at[s - 2, m, at], bg.at[slot], in_sem.at[slot]).start()

    def put(t, wait):
        slot = t % NB
        m, j, k = where(t)
        for mm in range(2):
            @pl.when(m == mm)
            def _():
                cp = pltpu.make_async_copy(bg.at[slot], w13.at[0, j, pl.ds(k * rows, rows), pl.ds(mm * f, f)], out_sem.at[slot])
                cp.wait() if wait else cp.start()

    def kept():
        for j in range(2):
            for p in range(PARTS):
                n = kdn.shape[1] // PARTS
                at = pl.ds(p * n, n)
                yield pltpu.make_async_copy(kdn.at[j, at], w2.at[0, j, at], k_sem.at[0, j, p])
                n = kup.shape[1] // PARTS
                yield pltpu.make_async_copy(kup.at[j, pl.ds(p * n, n)], w13.at[0, j, pl.ds(nup * rows + p * n, n), pl.ds(f, f)], k_sem.at[1, j, p])

    def tick(t, _):
        @pl.when(t < total)
        def _():
            @pl.when(t >= NB)
            def _():
                put(t - NB, True)
            fetch(t)

        @pl.when(t == AHEAD - 1)
        def _():
            for cp in kept():
                cp.start()
        u = t - AHEAD

        @pl.when(u >= 0)
        def _():
            slot = u % NB
            pltpu.make_async_copy(bg.at[slot], bg.at[slot], in_sem.at[slot]).wait()
            put(u, False)
        return 0
    lax.fori_loop(0, total + AHEAD, tick, 0)

    def drain(t, _):
        put(t, True)
        return 0
    lax.fori_loop(total - NB, total, drain, 0)
    for cp in kept():
        cp.wait()


def solution(mesh):
    def body(w_gate, w_up, w_down, place):
        d, f = w_gate.shape[2], w_gate.shape[3]
        bf16 = w_gate.dtype
        hbm = pl.BlockSpec(memory_space=pltpu.HBM)
        smem = pl.BlockSpec(memory_space=pltpu.SMEM)
        kept = pl.BlockSpec(memory_space=pltpu.VMEM)
        rg, rd = d // NG, f // ND
        in_hbm = functools.partial(pltpu.with_memory_space_constraint, memory_space=pltpu.HBM)
        vmem, dma = pltpu.VMEM, pltpu.SemaphoreType.DMA
        sgu, sd, kup, kdn = pl.pallas_call(
            _move,
            out_shape=(jax.ShapeDtypeStruct((4, 2, d, f), bf16), jax.ShapeDtypeStruct((4, f, d), bf16),
                       vmem((2, KEEP * rg, f), bf16), vmem((2, f, d), bf16)),
            in_specs=[smem, hbm, hbm, hbm],
            out_specs=(hbm, hbm, kept, kept),
            scratch_shapes=[vmem((NI, 2, rg, f), bf16), vmem((NO, rg, f), bf16), vmem((NI, 2, rd, d), bf16), vmem((NO, rd, d), bf16),
                            vmem((NI2, 2, rg, f), bf16), vmem((NO, rg, f), bf16), vmem((NI2, 2, rd, d), bf16), vmem((NO, rd, d), bf16),
                            vmem((NV, 2, 2, rg, f), bf16), vmem((NV, 2, 2, rd, d), bf16),
                            dma((NI, 2)), dma((NO,)), dma((NI2, 2)), dma((NO,)), dma((NV, 2, 2)), dma((3, 3)), dma((4, 2 * NG + ND))],
            compiler_params=pltpu.CompilerParams(collective_id=0, has_side_effects=True, vmem_limit_bytes=MOVE_VMEM),
            name="move",
        )(place, in_hbm(w_gate), in_hbm(w_up), in_hbm(w_down))
        return pl.pallas_call(
            _place,
            out_shape=(jax.ShapeDtypeStruct((1, 2, d, 2 * f), bf16), jax.ShapeDtypeStruct((1, 2, f, d), bf16)),
            in_specs=[smem, hbm, hbm, hbm, kept, kept],
            out_specs=(hbm, hbm),
            scratch_shapes=[vmem((NB, d // NP, f), bf16), dma((NB,)), dma((NB,)), dma((2, 2, PARTS))],
            compiler_params=pltpu.CompilerParams(vmem_limit_bytes=PLACE_VMEM),
            name="place",
        )(place, in_hbm(w_gate), in_hbm(w_up), in_hbm(sgu), kup, kdn)

    spec_in = P(None, "ep", None, None)
    spec_out = P(None, ("dp", "ep"), None, None)
    return jax.shard_map(body, mesh=mesh,
                         in_specs=(spec_in, spec_in, spec_in, P(None, None)),
                         out_specs=(spec_out, spec_out), check_vma=False)
```

```python
import functools

import jax
import jax.numpy as jnp
from jax import lax
from jax.experimental import pallas as pl
from jax.experimental.pallas import tpu as pltpu
from jax.sharding import PartitionSpec as P

C = 8
NI = 3
NO = 4
NV = 3
LAG = 4
LATE = ((4, 3), (3, 0), (0, 0), (0, 0))
DIRECT = 3
DELAY1 = 2
DELAY3 = 0
FIRST_KEPT = 72
BUF_P, BUF_Q, BUF_R, BUF_S = range(4)
MOVE_VMEM = 8 * 1024 * 1024
PLACE_VMEM = 8 * 1024 * 1024
STEP = 2


def _slot_of(place, a, g, j):
    return place[0, (a * 4 + g) * 2 + j] % 2


def _move(place, wg, wu, wd, st, kv0, kv1, i1, o1, i2, o2, ring, i1_sem, o1_sem, i2_sem, o2_sem, k_sem, fwd_sem, recv_sem):
    kv = (kv0, kv1)
    tiles = wg.shape[1]
    per = tiles // C
    total = 3 * per
    a = lax.axis_index("dp")
    g = lax.axis_index("ep")
    x, c = g // 2, g % 2

    def here(a2, c2):
        return (a == a2) & (c == c2)

    def dev(a2, c2):
        return (a2, 2 * x + c2)

    def within(q, fn, lo=0, hi=total):
        pl.when((q >= lo) & (q < hi))(fn)

    def local(q, fn, lo=0):
        for m, w in enumerate((wg, wu, wd)):
            within(q, lambda w=w, m=m: fn(lambda e: w.at[e, pl.ds((q - m * per) * C, C)]), jnp.maximum(lo, m * per), (m + 1) * per)

    def stage(b, q):
        return st.at[b, pl.ds(q * C, C)]

    def remote(src, dst, ssem, rsem, device):
        return pltpu.make_async_remote_copy(src_ref=src, dst_ref=dst, send_sem=ssem, recv_sem=rsem, device_id=device,
                                            device_id_type=pl.DeviceIdType.MESH)

    def wait_recv(b, q):
        within(q, lambda: remote(stage(b, q), stage(b, q), fwd_sem.at[0, 0], recv_sem.at[b, q], dev(a, 1 - c)).wait_recv())

    def forward(q, b, flow, device, hi=total):
        within(q, lambda: remote(stage(b, q), stage(b, q), fwd_sem.at[flow, q // per], recv_sem.at[b, q], device).start(), 0, hi)

    def wait_sent(flow, b, device, hi=total):
        for m in range(3):
            at = pl.ds(m * tiles, min(tiles, hi * C - m * tiles))
            remote(st.at[b, at], st.at[b, at], fwd_sem.at[flow, m], recv_sem.at[b, 0], device).wait_send()

    def pick_run(q, i, o, i_sem, o_sem, which, b, device, lo, hi):
        slot, oslot = q % NI, q % NO

        def free():
            remote(o.at[oslot], stage(b, q), o_sem.at[oslot], recv_sem.at[b, 0], device).wait_send()
        within(q, free, lo + NO, hi)

        def go():
            for e in range(2):
                pltpu.make_async_copy(st.at[0, pl.ds(0, C)], i.at[slot, e], i_sem.at[slot, e]).wait()

            def some(r, _):
                at = pl.ds(r * STEP, STEP)
                o[oslot, at] = jnp.where(which == 0, i[slot, 0, at], i[slot, 1, at])
                return 0
            lax.fori_loop(0, C // STEP, some, 0)
        within(q, go, lo, hi)

    def pick_send(q, o, o_sem, b, device, lo, hi):
        within(q, lambda: remote(o.at[q % NO], stage(b, q), o_sem.at[q % NO], recv_sem.at[b, q], device).start(), lo, hi)

    def pick_drain(o, o_sem, b, device, lo, hi):
        for n in range(NO):
            q = hi - NO + n
            within(q, lambda: remote(o.at[q % NO], stage(b, q), o_sem.at[q % NO], recv_sem.at[b, 0], device).wait_send(), lo, hi)

    mirror = (a, 2 * (1 - x) + c)
    other = 2 * (1 - x)
    far = _slot_of(place, 2, other, 1), _slot_of(place, 1, other + 1, 1)
    which = jnp.where(c == 0, far[0], far[1])
    which = jnp.where(here(1, 0) | here(2, 1), 1 - which, which)
    which = jnp.where(here(0, 1), _slot_of(place, 0, other + 1, 1), which)
    is_src = (c == 0) & (a < 2) | (c == 1) & (a >= 2)
    lo = jnp.where(is_src, 0, jnp.where(here(0, 1) | here(3, 0), total - DIRECT, total))
    delay = jnp.where(is_src, 0, jnp.where(c == 1, DELAY1, DELAY3))
    b = jnp.where(is_src, a % 2, jnp.where(c == 1, BUF_R, BUF_P))

    def pick_start(q):
        def go(src):
            for e in range(2):
                pltpu.make_async_copy(src(e), i1.at[q % NI, e], i1_sem.at[q % NI, e]).start()
        local(q, go, lo)

    def pick(q):
        pick_run(q, i1, o1, i1_sem, o1_sem, which, b, mirror, lo, total)

    far_a, far_b = _slot_of(place, 2, 2 * x, 1), _slot_of(place, 1, 2 * x + 1, 1)
    which2 = jnp.where(_slot_of(place, 0, 2 * x + 1, 1) == far_b, 1, 0)
    short = total - DIRECT

    def second(u):
        pick_run(u - 1, i2, o2, i2_sem, o2_sem, which2, BUF_R, dev(0, 1), 0, short)
        wait_recv(BUF_P, u)
        wait_recv(BUF_Q, u)

        def go():
            for e, block in enumerate((BUF_P, BUF_Q)):
                pltpu.make_async_copy(stage(block, u), i2.at[u % NI, e], i2_sem.at[u % NI, e]).start()
        within(u, go, 0, short)
        pick_send(u - 1, o2, o2_sem, BUF_R, dev(0, 1), 0, short)

    flows = {
        (0, 0): (BUF_P, ((dev(1, 0), total), (dev(2, 0), total), (dev(0, 1), total))),
        (0, 1): (BUF_Q, ((dev(0, 0), total),)),
        (1, 0): (BUF_Q, ((dev(0, 1), total), (dev(3, 0), total))),
        (2, 0): (BUF_P, ((dev(3, 0), short),)),
        (3, 1): (BUF_Q, ((dev(2, 1), total), (dev(1, 1), total))),
    }
    late = {(0, 0): (BUF_Q, BUF_R, BUF_S), (0, 1): (BUF_P, BUF_R), (1, 0): (BUF_P,), (1, 1): (BUF_Q,), (3, 0): (BUF_P, BUF_Q)}

    own = (here(1, 1) | here(2, 0) | here(3, 1), here(3, 1))
    pairs = ((jnp.where(here(0, 0), BUF_R, BUF_P), jnp.where(here(0, 0), BUF_S, BUF_Q)),
             (jnp.where(here(0, 1), BUF_R, jnp.where(here(1, 1), BUF_Q, BUF_P)),
              jnp.where(here(0, 1), BUF_R, jnp.where(here(2, 0), BUF_P, BUF_Q))))
    kept = []
    for j in range(2):
        e = _slot_of(place, a, g, j)
        from_a = (c == 0) | (here(0, 1) if j == 0 else False)
        near = own[j] | (here(0, 0) if j == 0 else False)
        kept.append(jnp.where(near, e, jnp.where(from_a, jnp.where(e == far_a, 0, 1), jnp.where(e == far_b, 1, 0))))

    def keep_to(q, j, e):
        return kv[j].at[pl.ds((q - FIRST_KEPT) * C, C)] if e == 0 else ring.at[q % NV, j]

    def keep_start(q):
        for j in range(2):
            def fetch(src, j=j):
                for e in range(2):
                    pltpu.make_async_copy(src(e), keep_to(q, j, e), k_sem.at[q % NV, j, e]).start()

            @pl.when(own[j])
            def _():
                local(q, fetch, FIRST_KEPT)

            @pl.when(jnp.logical_not(own[j]))
            def _():
                within(q, lambda: fetch(lambda e: stage(pairs[j][e], q)), FIRST_KEPT)

    def keep_run(q):
        def go():
            for j in range(2):
                for e in range(2):
                    pltpu.make_async_copy(st.at[0, pl.ds(0, C)], keep_to(q, j, e), k_sem.at[q % NV, j, e]).wait()

                def some(r, _):
                    at = pl.ds((q - FIRST_KEPT) * C + r * STEP, STEP)
                    kv[j][at] = jnp.where(kept[j] == 0, kv[j][at], ring[q % NV, j, pl.ds(r * STEP, STEP)])
                    return 0
                lax.fori_loop(0, C // STEP, some, 0)
        within(q, go, FIRST_KEPT)

    barrier = pltpu.get_barrier_semaphore()

    def greet(*partners):
        for device in partners:
            pl.semaphore_signal(barrier, inc=1, device_id=device, device_id_type=pl.DeviceIdType.MESH)

    partners = {
        (0, 0): (mirror, dev(1, 0), dev(2, 0), dev(0, 1)),
        (0, 1): (mirror, dev(0, 0), dev(1, 0), dev(2, 1)),
        (1, 0): (mirror, dev(0, 0), dev(0, 1), dev(3, 0)),
        (1, 1): (dev(3, 1),),
        (2, 0): (dev(0, 0), dev(3, 0)),
        (2, 1): (mirror, dev(3, 1), dev(0, 1)),
        (3, 0): (mirror, dev(1, 0), dev(2, 0)),
        (3, 1): (mirror, dev(2, 1), dev(1, 1)),
    }
    for (a2, c2), devices in partners.items():
        pl.when(here(a2, c2))(functools.partial(greet, *devices))

    def early(t, _):
        pick_start(t - delay)
        return 0
    lax.fori_loop(0, 3, early, 0)
    pick(0 - delay)
    for (a2, c2), devices in partners.items():
        pl.when(here(a2, c2))(lambda devices=devices: pl.semaphore_wait(barrier, len(devices)))

    behind = jnp.int32(0)
    for a2, cores in enumerate(LATE):
        for c2, n in enumerate(cores):
            behind = jnp.where(here(a2, c2), n, behind)

    def tick(t, _):
        u = t - 3 - LAG
        pick_send(t - 3 - delay, o1, o1_sem, b, mirror, lo, total)
        pick_start(t - delay)
        pick(t - 2 - delay)

        @pl.when(here(0, 1))
        def _():
            q = t - 3

            def give(src):
                for e in range(2):
                    remote(src(e), stage(BUF_R + e, q), fwd_sem.at[1 + e, q // per], recv_sem.at[BUF_R + e, q], dev(0, 0)).start()
            local(q, give)

        @pl.when(here(2, 1))
        def _():
            second(u)

        for (a2, c2), (block, devices) in flows.items():
            @pl.when(here(a2, c2))
            def _():
                wait_recv(block, u)
                for flow, (device, hi) in enumerate(devices):
                    forward(u, block, flow, device, hi)

        v = u - behind
        for (a2, c2), blocks in late.items():
            @pl.when(here(a2, c2))
            def _():
                for block in blocks:
                    wait_recv(block, v)
        keep_start(v)
        keep_run(v - 2)
        return 0
    lax.fori_loop(3, total + 3 + LAG + max(map(max, LATE)) + 2, tick, 0)

    pick_drain(o1, o1_sem, b, mirror, lo, total)

    @pl.when(here(2, 1))
    def _():
        pick_drain(o2, o2_sem, BUF_R, dev(0, 1), 0, short)

    for (a2, c2), (block, devices) in flows.items():
        @pl.when(here(a2, c2))
        def _():
            for flow, (device, hi) in enumerate(devices):
                wait_sent(flow, block, device, hi)

    @pl.when(here(0, 1))
    def _():
        wait_sent(1, BUF_R, dev(0, 0))
        wait_sent(2, BUF_S, dev(0, 0))


T = 32
NB = 8
AHEAD = 4
PARTS = 4
SPREAD = 2


def _place(place, wg, wu, st, kv0, kv1, w13, w2, buf, in_sem, out_sem, k_sem):
    kv = (kv0, kv1)
    a = lax.axis_index("dp")
    g = lax.axis_index("ep")
    x, c = g // 2, g % 2
    tiles = wg.shape[1]
    wide = w13.shape[2] // 2
    rest = FIRST_KEPT * C
    n = rest // T
    total = 2 * n

    far_a, far_b = _slot_of(place, 2, 2 * x, 1), _slot_of(place, 1, 2 * x + 1, 1)

    def source(j):
        e = _slot_of(place, a, g, j)
        from_a = jnp.where(e == far_a, 2 + BUF_P, 2 + BUF_Q)
        from_b = jnp.where(e == far_b, 2 + BUF_Q, 2 + BUF_P)
        if j == 0:
            c0 = jnp.where(a == 0, 2 + BUF_R + e, jnp.where(a == 2, e, from_a))
            c1 = jnp.where(a == 0, from_a, jnp.where(a == 2, from_b, e))
        else:
            c0 = jnp.where(a == 2, 2 + BUF_P, from_a)
            c1 = jnp.where(a == 0, 2 + BUF_R, jnp.where(a == 3, e, jnp.where(a == 1, 2 + BUF_Q, from_b)))
        return jnp.where(c == 0, c0, c1)

    sources = [source(0), source(1)]

    def fetch(t):
        slot = t % NB
        s = jnp.where(t % 2 == 0, sources[0], sources[1])
        k = t // 2
        m = k * T // tiles
        for mm, w in enumerate((wg, wu)):
            @pl.when((s < 2) & (m == mm))
            def _():
                pltpu.make_async_copy(w.at[s, pl.ds(k * T - mm * tiles, T)], buf.at[slot], in_sem.at[slot]).start()

        @pl.when(s >= 2)
        def _():
            pltpu.make_async_copy(st.at[s - 2, pl.ds(k * T, T)], buf.at[slot], in_sem.at[slot]).start()

    def put(t):
        k = t // 2
        m = k * T // tiles
        return pltpu.make_async_copy(buf.at[t % NB], w13.at[t % 2, pl.ds(k * T - m * tiles, T), pl.ds(m * wide, wide)], out_sem.at[t % NB])

    def kept():
        for j in range(2):
            for m in range(2):
                low, high = max(rest, m * tiles), (m + 1) * tiles
                step = T * max(1, (high - low) // T // PARTS)
                for p, at in enumerate(range(low, high, step)):
                    size = min(step, high - at)
                    yield pltpu.make_async_copy(kv[j].at[pl.ds(at - rest, size)],
                                                w13.at[j, pl.ds(at - m * tiles, size), pl.ds(m * wide, wide)], k_sem.at[m, j, p])
            step = tiles // PARTS
            for p in range(PARTS):
                yield pltpu.make_async_copy(kv[j].at[pl.ds(2 * tiles - rest + p * step, step)], w2.at[j, pl.ds(p * step, step)], k_sem.at[2, j, p])

    def tick(t, _):
        @pl.when(t < total)
        def _():
            @pl.when(t >= NB)
            def _():
                put(t - NB).wait()
            fetch(t)

        for n, cp in enumerate(kept()):
            pl.when(t == AHEAD - 1 + n * SPREAD)(cp.start)
        u = t - AHEAD

        @pl.when(u >= 0)
        def _():
            slot = u % NB
            pltpu.make_async_copy(st.at[0, pl.ds(0, T)], buf.at[slot], in_sem.at[slot]).wait()
            put(u).start()
        return 0
    lax.fori_loop(0, total + AHEAD, tick, 0)

    def drain(t, _):
        put(t).wait()
        return 0
    lax.fori_loop(total - NB, total, drain, 0)
    for cp in kept():
        cp.wait()


def _tiles(w, wide):
    _, e, r, k = w.shape
    return w.reshape(e, r // 8, 8, k // 128, 128).transpose(0, 1, 3, 2, 4).reshape(e, -1, wide, 8, 128)


def solution(mesh):
    def body(w_gate, w_up, w_down, place):
        d, f = w_gate.shape[2], w_gate.shape[3]
        bf16 = w_gate.dtype
        wg, wu, wd = (pltpu.with_memory_space_constraint(_tiles(w, f // 128), pltpu.HBM) for w in (w_gate, w_up, w_down))
        tiles, row = wg.shape[1], wg.shape[2:]
        hbm = pl.BlockSpec(memory_space=pltpu.HBM)
        smem = pl.BlockSpec(memory_space=pltpu.SMEM)
        kept = pl.BlockSpec(memory_space=pltpu.VMEM)
        vmem, dma = pltpu.VMEM, pltpu.SemaphoreType.DMA
        shape = jax.ShapeDtypeStruct
        keep = vmem((3 * tiles - FIRST_KEPT * C, *row), bf16)
        st, kv0, kv1 = pl.pallas_call(
            _move,
            out_shape=(shape((4, 3 * tiles, *row), bf16), keep, keep),
            in_specs=[smem, hbm, hbm, hbm],
            out_specs=(hbm, kept, kept),
            scratch_shapes=[vmem((NI, 2, C, *row), bf16), vmem((NO, C, *row), bf16), vmem((NI, 2, C, *row), bf16),
                            vmem((NO, C, *row), bf16), vmem((NV, 2, C, *row), bf16), dma((NI, 2)), dma((NO,)), dma((NI, 2)),
                            dma((NO,)), dma((NV, 2, 2)), dma((3, 3)), dma((4, 3 * tiles // C))],
            compiler_params=pltpu.CompilerParams(collective_id=0, has_side_effects=True, vmem_limit_bytes=MOVE_VMEM),
            name="move",
        )(place, wg, wu, wd)
        w13, w2 = pl.pallas_call(
            _place,
            out_shape=(shape((2, d // 8, f // 64, 8, 128), bf16), shape((2, tiles, *row), bf16)),
            in_specs=[smem, hbm, hbm, hbm, kept, kept],
            out_specs=(hbm, hbm),
            scratch_shapes=[vmem((NB, T, *row), bf16), dma((NB,)), dma((NB,)), dma((3, 2, 2 * PARTS))],
            compiler_params=pltpu.CompilerParams(vmem_limit_bytes=PLACE_VMEM),
            name="place",
        )(place, wg, wu, pltpu.with_memory_space_constraint(st, pltpu.HBM), kv0, kv1)
        w13 = w13.transpose(0, 1, 3, 2, 4).reshape(1, 2, d, 2 * f)
        w2 = w2.reshape(2, f // 8, d // 128, 8, 128).transpose(0, 1, 3, 2, 4).reshape(1, 2, f, d)
        return w13, w2

    spec_in = P(None, "ep", None, None)
    spec_out = P(None, ("dp", "ep"), None, None)
    return jax.shard_map(body, mesh=mesh,
                         in_specs=(spec_in, spec_in, spec_in, P(None, None)),
                         out_specs=(spec_out, spec_out), check_vma=False)
```

```python
import functools

import jax
import jax.numpy as jnp
from jax import lax
from jax.experimental import pallas as pl
from jax.experimental.pallas import tpu as pltpu
from jax.sharding import PartitionSpec as P

C = 8
NI = 3
NO = 4
NV = 3
LAG = 4
LATE = ((4, 3), (3, 0), (0, 0), (0, 0))
DIRECT = 3
DELAY1 = 2
DELAY3 = 0
FIRST_KEPT = 72
BUF_P, BUF_Q, BUF_R, BUF_S = range(4)
MOVE_VMEM = 8 * 1024 * 1024
PLACE_VMEM = 8 * 1024 * 1024
STEP = 2


def _slot_of(place, a, g, j):
    return place[0, (a * 4 + g) * 2 + j] % 2


def _move(place, wg, wu, wd, st, kv0, kv1, i1, o1, i2, o2, ring, i1_sem, o1_sem, i2_sem, o2_sem, k_sem, fwd_sem, recv_sem):
    kv = (kv0, kv1)
    tiles = wg.shape[1]
    per = tiles // C
    total = 3 * per
    a = lax.axis_index("dp")
    g = lax.axis_index("ep")
    x, c = g // 2, g % 2

    def here(a2, c2):
        return (a == a2) & (c == c2)

    def dev(a2, c2):
        return (a2, 2 * x + c2)

    def within(q, fn, lo=0, hi=total):
        pl.when((q >= lo) & (q < hi))(fn)

    def local(q, fn, lo=0):
        for m, w in enumerate((wg, wu, wd)):
            within(q, lambda w=w, m=m: fn(lambda e: w.at[e, pl.ds((q - m * per) * C, C)]), jnp.maximum(lo, m * per), (m + 1) * per)

    def stage(b, q):
        return st.at[b, pl.ds(q * C, C)]

    def remote(src, dst, ssem, rsem, device):
        return pltpu.make_async_remote_copy(src_ref=src, dst_ref=dst, send_sem=ssem, recv_sem=rsem, device_id=device,
                                            device_id_type=pl.DeviceIdType.MESH)

    def wait_recv(b, q):
        within(q, lambda: remote(stage(b, q), stage(b, q), fwd_sem.at[0, 0], recv_sem.at[b, q], dev(a, 1 - c)).wait_recv())

    def forward(q, b, flow, device, hi=total):
        within(q, lambda: remote(stage(b, q), stage(b, q), fwd_sem.at[flow, q // per], recv_sem.at[b, q], device).start(), 0, hi)

    def wait_sent(flow, b, device, hi=total):
        for m in range(3):
            at = pl.ds(m * tiles, min(tiles, hi * C - m * tiles))
            remote(st.at[b, at], st.at[b, at], fwd_sem.at[flow, m], recv_sem.at[b, 0], device).wait_send()

    def pick_run(q, i, o, i_sem, o_sem, which, b, device, lo, hi):
        slot, oslot = q % NI, q % NO

        def free():
            remote(o.at[oslot], stage(b, q), o_sem.at[oslot], recv_sem.at[b, 0], device).wait_send()
        within(q, free, lo + NO, hi)

        def go():
            for e in range(2):
                pltpu.make_async_copy(st.at[0, pl.ds(0, C)], i.at[slot, e], i_sem.at[slot, e]).wait()

            def some(r, _):
                at = pl.ds(r * STEP, STEP)
                o[oslot, at] = jnp.where(which == 0, i[slot, 0, at], i[slot, 1, at])
                return 0
            lax.fori_loop(0, C // STEP, some, 0)
        within(q, go, lo, hi)

    def pick_send(q, o, o_sem, b, device, lo, hi):
        within(q, lambda: remote(o.at[q % NO], stage(b, q), o_sem.at[q % NO], recv_sem.at[b, q], device).start(), lo, hi)

    def pick_drain(o, o_sem, b, device, lo, hi):
        for n in range(NO):
            q = hi - NO + n
            within(q, lambda: remote(o.at[q % NO], stage(b, q), o_sem.at[q % NO], recv_sem.at[b, 0], device).wait_send(), lo, hi)

    mirror = (a, 2 * (1 - x) + c)
    other = 2 * (1 - x)
    far = _slot_of(place, 2, other, 1), _slot_of(place, 1, other + 1, 1)
    which = jnp.where(c == 0, far[0], far[1])
    which = jnp.where(here(1, 0) | here(2, 1), 1 - which, which)
    which = jnp.where(here(0, 1), _slot_of(place, 0, other + 1, 1), which)
    is_src = (c == 0) & (a < 2) | (c == 1) & (a >= 2)
    lo = jnp.where(is_src, 0, jnp.where(here(0, 1) | here(3, 0), total - DIRECT, total))
    delay = jnp.where(is_src, 0, jnp.where(c == 1, DELAY1, DELAY3))
    b = jnp.where(is_src, a % 2, jnp.where(c == 1, BUF_R, BUF_P))

    def pick_start(q):
        def go(src):
            for e in range(2):
                pltpu.make_async_copy(src(e), i1.at[q % NI, e], i1_sem.at[q % NI, e]).start()
        local(q, go, lo)

    def pick(q):
        pick_run(q, i1, o1, i1_sem, o1_sem, which, b, mirror, lo, total)

    far_a, far_b = _slot_of(place, 2, 2 * x, 1), _slot_of(place, 1, 2 * x + 1, 1)
    which2 = jnp.where(_slot_of(place, 0, 2 * x + 1, 1) == far_b, 1, 0)
    short = total - DIRECT

    def second(u):
        pick_send(u - 2, o2, o2_sem, BUF_R, dev(0, 1), 0, short)
        wait_recv(BUF_P, u)
        wait_recv(BUF_Q, u)
        pick_run(u - 1, i2, o2, i2_sem, o2_sem, which2, BUF_R, dev(0, 1), 0, short)

        def go():
            for e, block in enumerate((BUF_P, BUF_Q)):
                pltpu.make_async_copy(stage(block, u), i2.at[u % NI, e], i2_sem.at[u % NI, e]).start()
        within(u, go, 0, short)

    flows = {
        (0, 0): (BUF_P, ((dev(1, 0), total), (dev(2, 0), total), (dev(0, 1), total))),
        (0, 1): (BUF_Q, ((dev(0, 0), total),)),
        (1, 0): (BUF_Q, ((dev(0, 1), total), (dev(3, 0), total))),
        (2, 0): (BUF_P, ((dev(3, 0), short),)),
        (3, 1): (BUF_Q, ((dev(2, 1), total), (dev(1, 1), total))),
    }
    late = {(0, 0): (BUF_Q, BUF_R, BUF_S), (0, 1): (BUF_P, BUF_R), (1, 0): (BUF_P,), (1, 1): (BUF_Q,), (3, 0): (BUF_P, BUF_Q)}

    own = (here(1, 1) | here(2, 0) | here(3, 1), here(3, 1))
    pairs = ((jnp.where(here(0, 0), BUF_R, BUF_P), jnp.where(here(0, 0), BUF_S, BUF_Q)),
             (jnp.where(here(0, 1), BUF_R, jnp.where(here(1, 1), BUF_Q, BUF_P)),
              jnp.where(here(0, 1), BUF_R, jnp.where(here(2, 0), BUF_P, BUF_Q))))
    kept = []
    for j in range(2):
        e = _slot_of(place, a, g, j)
        from_a = (c == 0) | (here(0, 1) if j == 0 else False)
        near = own[j] | (here(0, 0) if j == 0 else False)
        kept.append(jnp.where(near, e, jnp.where(from_a, jnp.where(e == far_a, 0, 1), jnp.where(e == far_b, 1, 0))))

    def keep_to(q, j, e):
        return kv[j].at[pl.ds((q - FIRST_KEPT) * C, C)] if e == 0 else ring.at[q % NV, j]

    def keep_start(q):
        for j in range(2):
            def fetch(src, j=j):
                for e in range(2):
                    pltpu.make_async_copy(src(e), keep_to(q, j, e), k_sem.at[q % NV, j, e]).start()

            @pl.when(own[j])
            def _():
                local(q, fetch, FIRST_KEPT)

            @pl.when(jnp.logical_not(own[j]))
            def _():
                within(q, lambda: fetch(lambda e: stage(pairs[j][e], q)), FIRST_KEPT)

    def keep_run(q):
        def go():
            for j in range(2):
                for e in range(2):
                    pltpu.make_async_copy(st.at[0, pl.ds(0, C)], keep_to(q, j, e), k_sem.at[q % NV, j, e]).wait()

                def some(r, _):
                    at = pl.ds((q - FIRST_KEPT) * C + r * STEP, STEP)
                    kv[j][at] = jnp.where(kept[j] == 0, kv[j][at], ring[q % NV, j, pl.ds(r * STEP, STEP)])
                    return 0
                lax.fori_loop(0, C // STEP, some, 0)
        within(q, go, FIRST_KEPT)

    barrier = pltpu.get_barrier_semaphore()

    def greet(*partners):
        for device in partners:
            pl.semaphore_signal(barrier, inc=1, device_id=device, device_id_type=pl.DeviceIdType.MESH)

    partners = {
        (0, 0): (mirror, dev(1, 0), dev(2, 0), dev(0, 1)),
        (0, 1): (mirror, dev(0, 0), dev(1, 0), dev(2, 1)),
        (1, 0): (mirror, dev(0, 0), dev(0, 1), dev(3, 0)),
        (1, 1): (dev(3, 1),),
        (2, 0): (dev(0, 0), dev(3, 0)),
        (2, 1): (mirror, dev(3, 1), dev(0, 1)),
        (3, 0): (mirror, dev(1, 0), dev(2, 0)),
        (3, 1): (mirror, dev(2, 1), dev(1, 1)),
    }
    for (a2, c2), devices in partners.items():
        pl.when(here(a2, c2))(functools.partial(greet, *devices))

    def early(t, _):
        pick_start(t - delay)
        return 0
    lax.fori_loop(0, 3, early, 0)
    pick(0 - delay)
    for (a2, c2), devices in partners.items():
        pl.when(here(a2, c2))(lambda devices=devices: pl.semaphore_wait(barrier, len(devices)))

    behind = jnp.int32(0)
    for a2, cores in enumerate(LATE):
        for c2, n in enumerate(cores):
            behind = jnp.where(here(a2, c2), n, behind)

    def tick(t, _):
        u = t - 3 - LAG
        pick_send(t - 3 - delay, o1, o1_sem, b, mirror, lo, total)
        pick_start(t - delay)
        pick(t - 2 - delay)

        @pl.when(here(0, 1))
        def _():
            q = t - 3

            def give(src):
                for e in range(2):
                    remote(src(e), stage(BUF_R + e, q), fwd_sem.at[1 + e, q // per], recv_sem.at[BUF_R + e, q], dev(0, 0)).start()
            local(q, give)

        @pl.when(here(2, 1))
        def _():
            second(u)

        for (a2, c2), (block, devices) in flows.items():
            @pl.when(here(a2, c2))
            def _():
                wait_recv(block, u)
                for flow, (device, hi) in enumerate(devices):
                    forward(u, block, flow, device, hi)

        v = u - behind
        for (a2, c2), blocks in late.items():
            @pl.when(here(a2, c2))
            def _():
                for block in blocks:
                    wait_recv(block, v)
        keep_start(v)
        keep_run(v - 2)
        return 0
    lax.fori_loop(3, total + 3 + LAG + max(map(max, LATE)) + 2, tick, 0)

    pick_drain(o1, o1_sem, b, mirror, lo, total)

    @pl.when(here(2, 1))
    def _():
        pick_drain(o2, o2_sem, BUF_R, dev(0, 1), 0, short)

    for (a2, c2), (block, devices) in flows.items():
        @pl.when(here(a2, c2))
        def _():
            for flow, (device, hi) in enumerate(devices):
                wait_sent(flow, block, device, hi)

    @pl.when(here(0, 1))
    def _():
        wait_sent(1, BUF_R, dev(0, 0))
        wait_sent(2, BUF_S, dev(0, 0))


T = 32
NB = 8
AHEAD = 4
PARTS = 4
SPREAD = 2


def _place(place, wg, wu, st, kv0, kv1, w13, w2, buf, in_sem, out_sem, k_sem):
    kv = (kv0, kv1)
    a = lax.axis_index("dp")
    g = lax.axis_index("ep")
    x, c = g // 2, g % 2
    tiles = wg.shape[1]
    wide = w13.shape[2] // 2
    rest = FIRST_KEPT * C
    n = rest // T
    total = 2 * n

    far_a, far_b = _slot_of(place, 2, 2 * x, 1), _slot_of(place, 1, 2 * x + 1, 1)

    def source(j):
        e = _slot_of(place, a, g, j)
        from_a = jnp.where(e == far_a, 2 + BUF_P, 2 + BUF_Q)
        from_b = jnp.where(e == far_b, 2 + BUF_Q, 2 + BUF_P)
        if j == 0:
            c0 = jnp.where(a == 0, 2 + BUF_R + e, jnp.where(a == 2, e, from_a))
            c1 = jnp.where(a == 0, from_a, jnp.where(a == 2, from_b, e))
        else:
            c0 = jnp.where(a == 2, 2 + BUF_P, from_a)
            c1 = jnp.where(a == 0, 2 + BUF_R, jnp.where(a == 3, e, jnp.where(a == 1, 2 + BUF_Q, from_b)))
        return jnp.where(c == 0, c0, c1)

    sources = [source(0), source(1)]

    def fetch(t):
        slot = t % NB
        s = jnp.where(t % 2 == 0, sources[0], sources[1])
        k = t // 2
        m = k * T // tiles
        for mm, w in enumerate((wg, wu)):
            @pl.when((s < 2) & (m == mm))
            def _():
                pltpu.make_async_copy(w.at[s, pl.ds(k * T - mm * tiles, T)], buf.at[slot], in_sem.at[slot]).start()

        @pl.when(s >= 2)
        def _():
            pltpu.make_async_copy(st.at[s - 2, pl.ds(k * T, T)], buf.at[slot], in_sem.at[slot]).start()

    def put(t):
        k = t // 2
        m = k * T // tiles
        return pltpu.make_async_copy(buf.at[t % NB], w13.at[t % 2, pl.ds(k * T - m * tiles, T), pl.ds(m * wide, wide)], out_sem.at[t % NB])

    def kept():
        for j in range(2):
            for m in range(2):
                low, high = max(rest, m * tiles), (m + 1) * tiles
                step = T * max(1, (high - low) // T // PARTS)
                for p, at in enumerate(range(low, high, step)):
                    size = min(step, high - at)
                    yield pltpu.make_async_copy(kv[j].at[pl.ds(at - rest, size)],
                                                w13.at[j, pl.ds(at - m * tiles, size), pl.ds(m * wide, wide)], k_sem.at[m, j, p])
            step = tiles // PARTS
            for p in range(PARTS):
                yield pltpu.make_async_copy(kv[j].at[pl.ds(2 * tiles - rest + p * step, step)], w2.at[j, pl.ds(p * step, step)], k_sem.at[2, j, p])

    def tick(t, _):
        @pl.when(t < total)
        def _():
            @pl.when(t >= NB)
            def _():
                put(t - NB).wait()
            fetch(t)

        for n, cp in enumerate(kept()):
            pl.when(t == AHEAD - 1 + n * SPREAD)(cp.start)
        u = t - AHEAD

        @pl.when(u >= 0)
        def _():
            slot = u % NB
            pltpu.make_async_copy(st.at[0, pl.ds(0, T)], buf.at[slot], in_sem.at[slot]).wait()
            put(u).start()
        return 0
    lax.fori_loop(0, total + AHEAD, tick, 0)

    def drain(t, _):
        put(t).wait()
        return 0
    lax.fori_loop(total - NB, total, drain, 0)
    for cp in kept():
        cp.wait()


def _tiles(w, wide):
    _, e, r, k = w.shape
    return w.reshape(e, r // 8, 8, k // 128, 128).transpose(0, 1, 3, 2, 4).reshape(e, -1, wide, 8, 128)


def solution(mesh):
    def body(w_gate, w_up, w_down, place):
        d, f = w_gate.shape[2], w_gate.shape[3]
        bf16 = w_gate.dtype
        wg, wu, wd = (pltpu.with_memory_space_constraint(_tiles(w, f // 128), pltpu.HBM) for w in (w_gate, w_up, w_down))
        tiles, row = wg.shape[1], wg.shape[2:]
        hbm = pl.BlockSpec(memory_space=pltpu.HBM)
        smem = pl.BlockSpec(memory_space=pltpu.SMEM)
        kept = pl.BlockSpec(memory_space=pltpu.VMEM)
        vmem, dma = pltpu.VMEM, pltpu.SemaphoreType.DMA
        shape = jax.ShapeDtypeStruct
        keep = vmem((3 * tiles - FIRST_KEPT * C, *row), bf16)
        st, kv0, kv1 = pl.pallas_call(
            _move,
            out_shape=(shape((4, 3 * tiles, *row), bf16), keep, keep),
            in_specs=[smem, hbm, hbm, hbm],
            out_specs=(hbm, kept, kept),
            scratch_shapes=[vmem((NI, 2, C, *row), bf16), vmem((NO, C, *row), bf16), vmem((NI, 2, C, *row), bf16),
                            vmem((NO, C, *row), bf16), vmem((NV, 2, C, *row), bf16), dma((NI, 2)), dma((NO,)), dma((NI, 2)),
                            dma((NO,)), dma((NV, 2, 2)), dma((3, 3)), dma((4, 3 * tiles // C))],
            compiler_params=pltpu.CompilerParams(collective_id=0, has_side_effects=True, vmem_limit_bytes=MOVE_VMEM),
            name="move",
        )(place, wg, wu, wd)
        w13, w2 = pl.pallas_call(
            _place,
            out_shape=(shape((2, d // 8, f // 64, 8, 128), bf16), shape((2, tiles, *row), bf16)),
            in_specs=[smem, hbm, hbm, hbm, kept, kept],
            out_specs=(hbm, hbm),
            scratch_shapes=[vmem((NB, T, *row), bf16), dma((NB,)), dma((NB,)), dma((3, 2, 2 * PARTS))],
            compiler_params=pltpu.CompilerParams(vmem_limit_bytes=PLACE_VMEM),
            name="place",
        )(place, wg, wu, pltpu.with_memory_space_constraint(st, pltpu.HBM), kv0, kv1)
        w13 = w13.transpose(0, 1, 3, 2, 4).reshape(1, 2, d, 2 * f)
        w2 = w2.reshape(2, f // 8, d // 128, 8, 128).transpose(0, 1, 3, 2, 4).reshape(1, 2, f, d)
        return w13, w2

    spec_in = P(None, "ep", None, None)
    spec_out = P(None, ("dp", "ep"), None, None)
    return jax.shard_map(body, mesh=mesh,
                         in_specs=(spec_in, spec_in, spec_in, P(None, None)),
                         out_specs=(spec_out, spec_out), check_vma=False)
```

```python
import functools

import jax
import jax.numpy as jnp
from jax import lax
from jax.experimental import pallas as pl
from jax.experimental.pallas import tpu as pltpu
from jax.sharding import PartitionSpec as P

C = 8
NI = 3
NO = 4
NV = 3
LAG = 4
LATE = ((4, 3), (3, 0), (0, 0), (0, 0))
DIRECT = 3
DELAY1 = 2
DELAY3 = 0
FIRST_KEPT = 68
LAST = 4
BUF_P, BUF_Q, BUF_R, BUF_S = range(4)
MOVE_VMEM = 8 * 1024 * 1024
PLACE_VMEM = 8 * 1024 * 1024
STEP = 2


def _slot_of(place, a, g, j):
    return place[0, (a * 4 + g) * 2 + j] % 2


def _move(place, wg, wu, wd, st, kv0, kv1, i1, o1, i2, o2, ring, i1_sem, o1_sem, i2_sem, o2_sem, k_sem, fwd_sem, recv_sem):
    kv = (kv0, kv1)
    tiles = wg.shape[1]
    per = tiles // C
    total = 3 * per
    a = lax.axis_index("dp")
    g = lax.axis_index("ep")
    x, c = g // 2, g % 2

    def here(a2, c2):
        return (a == a2) & (c == c2)

    def dev(a2, c2):
        return (a2, 2 * x + c2)

    def within(q, fn, lo=0, hi=total):
        pl.when((q >= lo) & (q < hi))(fn)

    def local(q, fn, lo=0):
        for m, w in enumerate((wg, wu, wd)):
            within(q, lambda w=w, m=m: fn(lambda e: w.at[e, pl.ds((q - m * per) * C, C)]), jnp.maximum(lo, m * per), (m + 1) * per)

    def stage(b, q):
        return st.at[b, pl.ds(q * C, C)]

    def remote(src, dst, ssem, rsem, device):
        return pltpu.make_async_remote_copy(src_ref=src, dst_ref=dst, send_sem=ssem, recv_sem=rsem, device_id=device,
                                            device_id_type=pl.DeviceIdType.MESH)

    def wait_recv(b, q):
        within(q, lambda: remote(stage(b, q), stage(b, q), fwd_sem.at[0, 0], recv_sem.at[b, q], dev(a, 1 - c)).wait_recv())

    def forward(q, b, flow, device, hi=total):
        within(q, lambda: remote(stage(b, q), stage(b, q), fwd_sem.at[flow, q // per], recv_sem.at[b, q], device).start(), 0, hi)

    def wait_sent(flow, b, device, hi=total):
        for m in range(3):
            at = pl.ds(m * tiles, min(tiles, hi * C - m * tiles))
            remote(st.at[b, at], st.at[b, at], fwd_sem.at[flow, m], recv_sem.at[b, 0], device).wait_send()

    def pick_run(q, i, o, i_sem, o_sem, which, b, device, lo, hi):
        slot, oslot = q % NI, q % NO

        def free():
            remote(o.at[oslot], stage(b, q), o_sem.at[oslot], recv_sem.at[b, 0], device).wait_send()
        within(q, free, lo + NO, hi)

        def go():
            for e in range(2):
                pltpu.make_async_copy(st.at[0, pl.ds(0, C)], i.at[slot, e], i_sem.at[slot, e]).wait()

            def some(r, _):
                at = pl.ds(r * STEP, STEP)
                o[oslot, at] = jnp.where(which == 0, i[slot, 0, at], i[slot, 1, at])
                return 0
            lax.fori_loop(0, C // STEP, some, 0)
        within(q, go, lo, hi)

    def pick_send(q, o, o_sem, b, device, lo, hi):
        within(q, lambda: remote(o.at[q % NO], stage(b, q), o_sem.at[q % NO], recv_sem.at[b, q], device).start(), lo, hi)

    def pick_drain(o, o_sem, b, device, lo, hi):
        for n in range(NO):
            q = hi - NO + n
            within(q, lambda: remote(o.at[q % NO], stage(b, q), o_sem.at[q % NO], recv_sem.at[b, 0], device).wait_send(), lo, hi)

    mirror = (a, 2 * (1 - x) + c)
    other = 2 * (1 - x)
    far = _slot_of(place, 2, other, 1), _slot_of(place, 1, other + 1, 1)
    which = jnp.where(c == 0, far[0], far[1])
    which = jnp.where(here(1, 0) | here(2, 1), 1 - which, which)
    which = jnp.where(here(0, 1), _slot_of(place, 0, other + 1, 1), which)
    is_src = (c == 0) & (a < 2) | (c == 1) & (a >= 2)
    lo = jnp.where(is_src, 0, jnp.where(here(0, 1) | here(3, 0), total - DIRECT, total))
    delay = jnp.where(is_src, 0, jnp.where(c == 1, DELAY1, DELAY3))
    b = jnp.where(is_src, a % 2, jnp.where(c == 1, BUF_R, BUF_P))

    def pick_start(q):
        def go(src):
            for e in range(2):
                pltpu.make_async_copy(src(e), i1.at[q % NI, e], i1_sem.at[q % NI, e]).start()
        local(q, go, lo)

    def pick(q):
        pick_run(q, i1, o1, i1_sem, o1_sem, which, b, mirror, lo, total)

    far_a, far_b = _slot_of(place, 2, 2 * x, 1), _slot_of(place, 1, 2 * x + 1, 1)
    which2 = jnp.where(_slot_of(place, 0, 2 * x + 1, 1) == far_b, 1, 0)
    short = total - DIRECT

    def second(u):
        pick_send(u - 2, o2, o2_sem, BUF_R, dev(0, 1), 0, short)
        wait_recv(BUF_P, u)
        wait_recv(BUF_Q, u)
        pick_run(u - 1, i2, o2, i2_sem, o2_sem, which2, BUF_R, dev(0, 1), 0, short)

        def go():
            for e, block in enumerate((BUF_P, BUF_Q)):
                pltpu.make_async_copy(stage(block, u), i2.at[u % NI, e], i2_sem.at[u % NI, e]).start()
        within(u, go, 0, short)

    flows = {
        (0, 0): (BUF_P, ((dev(1, 0), total), (dev(2, 0), total), (dev(0, 1), total))),
        (0, 1): (BUF_Q, ((dev(0, 0), total),)),
        (1, 0): (BUF_Q, ((dev(0, 1), total), (dev(3, 0), total))),
        (2, 0): (BUF_P, ((dev(3, 0), short),)),
        (3, 1): (BUF_Q, ((dev(2, 1), total), (dev(1, 1), total))),
    }
    late = {(0, 0): (BUF_Q, BUF_R, BUF_S), (0, 1): (BUF_P, BUF_R), (1, 0): (BUF_P,), (1, 1): (BUF_Q,), (3, 0): (BUF_P, BUF_Q)}

    own = (here(1, 1) | here(2, 0) | here(3, 1), here(3, 1))
    pairs = ((jnp.where(here(0, 0), BUF_R, BUF_P), jnp.where(here(0, 0), BUF_S, BUF_Q)),
             (jnp.where(here(0, 1), BUF_R, jnp.where(here(1, 1), BUF_Q, BUF_P)),
              jnp.where(here(0, 1), BUF_R, jnp.where(here(2, 0), BUF_P, BUF_Q))))
    kept = []
    for j in range(2):
        e = _slot_of(place, a, g, j)
        from_a = (c == 0) | (here(0, 1) if j == 0 else False)
        near = own[j] | (here(0, 0) if j == 0 else False)
        kept.append(jnp.where(near, e, jnp.where(from_a, jnp.where(e == far_a, 0, 1), jnp.where(e == far_b, 1, 0))))

    def keep_to(q, j, e):
        return kv[j].at[pl.ds((q - FIRST_KEPT) * C, C)] if e == 0 else ring.at[q % NV, j]

    def keep_start(q):
        for j in range(2):
            def fetch(src, j=j):
                for e in range(2):
                    pltpu.make_async_copy(src(e), keep_to(q, j, e), k_sem.at[q % NV, j, e]).start()

            @pl.when(own[j])
            def _():
                local(jnp.where(q < total - LAST, q, -1), fetch, FIRST_KEPT)

            @pl.when(jnp.logical_not(own[j]))
            def _():
                within(q, lambda: fetch(lambda e: stage(pairs[j][e], q)), FIRST_KEPT, total - LAST)

    def keep_run(q):
        def go():
            for j in range(2):
                for e in range(2):
                    pltpu.make_async_copy(st.at[0, pl.ds(0, C)], keep_to(q, j, e), k_sem.at[q % NV, j, e]).wait()

                def some(r, _):
                    at = pl.ds((q - FIRST_KEPT) * C + r * STEP, STEP)
                    kv[j][at] = jnp.where(kept[j] == 0, kv[j][at], ring[q % NV, j, pl.ds(r * STEP, STEP)])
                    return 0
                lax.fori_loop(0, C // STEP, some, 0)
        within(q, go, FIRST_KEPT, total - LAST)

    barrier = pltpu.get_barrier_semaphore()

    def greet(*partners):
        for device in partners:
            pl.semaphore_signal(barrier, inc=1, device_id=device, device_id_type=pl.DeviceIdType.MESH)

    partners = {
        (0, 0): (mirror, dev(1, 0), dev(2, 0), dev(0, 1)),
        (0, 1): (mirror, dev(0, 0), dev(1, 0), dev(2, 1)),
        (1, 0): (mirror, dev(0, 0), dev(0, 1), dev(3, 0)),
        (1, 1): (dev(3, 1),),
        (2, 0): (dev(0, 0), dev(3, 0)),
        (2, 1): (mirror, dev(3, 1), dev(0, 1)),
        (3, 0): (mirror, dev(1, 0), dev(2, 0)),
        (3, 1): (mirror, dev(2, 1), dev(1, 1)),
    }
    for (a2, c2), devices in partners.items():
        pl.when(here(a2, c2))(functools.partial(greet, *devices))

    def early(t, _):
        pick_start(t - delay)
        return 0
    lax.fori_loop(0, 3, early, 0)
    pick(0 - delay)
    for (a2, c2), devices in partners.items():
        pl.when(here(a2, c2))(lambda devices=devices: pl.semaphore_wait(barrier, len(devices)))

    behind = jnp.int32(0)
    for a2, cores in enumerate(LATE):
        for c2, n in enumerate(cores):
            behind = jnp.where(here(a2, c2), n, behind)

    def tick(t, _):
        u = t - 3 - LAG
        pick_send(t - 3 - delay, o1, o1_sem, b, mirror, lo, total)
        pick_start(t - delay)
        pick(t - 2 - delay)

        @pl.when(here(0, 1))
        def _():
            q = t - 3

            def give(src):
                for e in range(2):
                    remote(src(e), stage(BUF_R + e, q), fwd_sem.at[1 + e, q // per], recv_sem.at[BUF_R + e, q], dev(0, 0)).start()
            local(q, give)

        @pl.when(here(2, 1))
        def _():
            second(u)

        for (a2, c2), (block, devices) in flows.items():
            @pl.when(here(a2, c2))
            def _():
                wait_recv(block, u)
                for flow, (device, hi) in enumerate(devices):
                    forward(u, block, flow, device, hi)

        v = u - behind
        for (a2, c2), blocks in late.items():
            @pl.when(here(a2, c2))
            def _():
                for block in blocks:
                    wait_recv(block, v)
        keep_start(v)
        keep_run(v - 2)
        return 0
    lax.fori_loop(3, total + 3 + LAG + max(map(max, LATE)), tick, 0)

    pick_drain(o1, o1_sem, b, mirror, lo, total)

    @pl.when(here(2, 1))
    def _():
        pick_drain(o2, o2_sem, BUF_R, dev(0, 1), 0, short)

    for (a2, c2), (block, devices) in flows.items():
        @pl.when(here(a2, c2))
        def _():
            for flow, (device, hi) in enumerate(devices):
                wait_sent(flow, block, device, hi)

    @pl.when(here(0, 1))
    def _():
        wait_sent(1, BUF_R, dev(0, 0))
        wait_sent(2, BUF_S, dev(0, 0))


T = 32
NB = 8
AHEAD = 4
PARTS = 4
SPREAD = 2


def _place(place, wg, wu, wd, st, kv0, kv1, w13, w2, buf, in_sem, out_sem, k_sem):
    kv = (kv0, kv1)
    a = lax.axis_index("dp")
    g = lax.axis_index("ep")
    x, c = g // 2, g % 2
    tiles = wg.shape[1]
    wide = w13.shape[2] // 2
    rest = FIRST_KEPT * C
    end = 3 * tiles - LAST * C
    n = rest // T
    total = 2 * (n + 1)

    far_a, far_b = _slot_of(place, 2, 2 * x, 1), _slot_of(place, 1, 2 * x + 1, 1)

    def source(j):
        e = _slot_of(place, a, g, j)
        from_a = jnp.where(e == far_a, 2 + BUF_P, 2 + BUF_Q)
        from_b = jnp.where(e == far_b, 2 + BUF_Q, 2 + BUF_P)
        if j == 0:
            c0 = jnp.where(a == 0, 2 + BUF_R + e, jnp.where(a == 2, e, from_a))
            c1 = jnp.where(a == 0, from_a, jnp.where(a == 2, from_b, e))
        else:
            c0 = jnp.where(a == 2, 2 + BUF_P, from_a)
            c1 = jnp.where(a == 0, 2 + BUF_R, jnp.where(a == 3, e, jnp.where(a == 1, 2 + BUF_Q, from_b)))
        return jnp.where(c == 0, c0, c1)

    sources = [source(0), source(1)]

    def fetch(t):
        slot = t % NB
        s = jnp.where(t % 2 == 0, sources[0], sources[1])
        k = t // 2
        low = jnp.where(k < n, k * T, end)
        m = low // tiles
        for mm, w in enumerate((wg, wu, wd)):
            @pl.when((s < 2) & (m == mm))
            def _():
                pltpu.make_async_copy(w.at[s, pl.ds(low - mm * tiles, T)], buf.at[slot], in_sem.at[slot]).start()

        @pl.when(s >= 2)
        def _():
            pltpu.make_async_copy(st.at[s - 2, pl.ds(low, T)], buf.at[slot], in_sem.at[slot]).start()

    def put(t, wait):
        k = t // 2
        m = k * T // tiles
        src, sem = buf.at[t % NB], out_sem.at[t % NB]

        @pl.when(k < n)
        def _():
            cp = pltpu.make_async_copy(src, w13.at[t % 2, pl.ds(k * T - m * tiles, T), pl.ds(m * wide, wide)], sem)
            cp.wait() if wait else cp.start()

        @pl.when(k == n)
        def _():
            cp = pltpu.make_async_copy(src, w2.at[t % 2, pl.ds(end - 2 * tiles, T)], sem)
            cp.wait() if wait else cp.start()

    def kept():
        for j in range(2):
            for m in range(2):
                low, high = max(rest, m * tiles), (m + 1) * tiles
                step = T * max(1, (high - low) // T // PARTS)
                for p, at in enumerate(range(low, high, step)):
                    size = min(step, high - at)
                    yield pltpu.make_async_copy(kv[j].at[pl.ds(at - rest, size)],
                                                w13.at[j, pl.ds(at - m * tiles, size), pl.ds(m * wide, wide)], k_sem.at[m, j, p])
            step = tiles // PARTS
            for p in range(PARTS):
                size = min(step, end - 2 * tiles - p * step)
                yield pltpu.make_async_copy(kv[j].at[pl.ds(2 * tiles - rest + p * step, size)], w2.at[j, pl.ds(p * step, size)], k_sem.at[2, j, p])

    def tick(t, _):
        @pl.when(t < total)
        def _():
            @pl.when(t >= NB)
            def _():
                put(t - NB, True)
            fetch(t)

        for n, cp in enumerate(kept()):
            pl.when(t == AHEAD - 1 + n * SPREAD)(cp.start)
        u = t - AHEAD

        @pl.when(u >= 0)
        def _():
            slot = u % NB
            pltpu.make_async_copy(st.at[0, pl.ds(0, T)], buf.at[slot], in_sem.at[slot]).wait()
            put(u, False)
        return 0
    lax.fori_loop(0, total + AHEAD, tick, 0)

    def drain(t, _):
        put(t, True)
        return 0
    lax.fori_loop(total - NB, total, drain, 0)
    for cp in kept():
        cp.wait()


def _tiles(w, wide):
    _, e, r, k = w.shape
    return w.reshape(e, r // 8, 8, k // 128, 128).transpose(0, 1, 3, 2, 4).reshape(e, -1, wide, 8, 128)


def solution(mesh):
    def body(w_gate, w_up, w_down, place):
        d, f = w_gate.shape[2], w_gate.shape[3]
        bf16 = w_gate.dtype
        wg, wu, wd = (pltpu.with_memory_space_constraint(_tiles(w, f // 128), pltpu.HBM) for w in (w_gate, w_up, w_down))
        tiles, row = wg.shape[1], wg.shape[2:]
        hbm = pl.BlockSpec(memory_space=pltpu.HBM)
        smem = pl.BlockSpec(memory_space=pltpu.SMEM)
        kept = pl.BlockSpec(memory_space=pltpu.VMEM)
        vmem, dma = pltpu.VMEM, pltpu.SemaphoreType.DMA
        shape = jax.ShapeDtypeStruct
        keep = vmem((3 * tiles - (FIRST_KEPT + LAST) * C, *row), bf16)
        st, kv0, kv1 = pl.pallas_call(
            _move,
            out_shape=(shape((4, 3 * tiles, *row), bf16), keep, keep),
            in_specs=[smem, hbm, hbm, hbm],
            out_specs=(hbm, kept, kept),
            scratch_shapes=[vmem((NI, 2, C, *row), bf16), vmem((NO, C, *row), bf16), vmem((NI, 2, C, *row), bf16),
                            vmem((NO, C, *row), bf16), vmem((NV, 2, C, *row), bf16), dma((NI, 2)), dma((NO,)), dma((NI, 2)),
                            dma((NO,)), dma((NV, 2, 2)), dma((3, 3)), dma((4, 3 * tiles // C))],
            compiler_params=pltpu.CompilerParams(collective_id=0, has_side_effects=True, vmem_limit_bytes=MOVE_VMEM),
            name="move",
        )(place, wg, wu, wd)
        w13, w2 = pl.pallas_call(
            _place,
            out_shape=(shape((2, d // 8, f // 64, 8, 128), bf16), shape((2, tiles, *row), bf16)),
            in_specs=[smem, hbm, hbm, hbm, hbm, kept, kept],
            out_specs=(hbm, hbm),
            scratch_shapes=[vmem((NB, T, *row), bf16), dma((NB,)), dma((NB,)), dma((3, 2, 2 * PARTS))],
            compiler_params=pltpu.CompilerParams(vmem_limit_bytes=PLACE_VMEM),
            name="place",
        )(place, wg, wu, wd, pltpu.with_memory_space_constraint(st, pltpu.HBM), kv0, kv1)
        w13 = w13.transpose(0, 1, 3, 2, 4).reshape(1, 2, d, 2 * f)
        w2 = w2.reshape(2, f // 8, d // 128, 8, 128).transpose(0, 1, 3, 2, 4).reshape(1, 2, f, d)
        return w13, w2

    spec_in = P(None, "ep", None, None)
    spec_out = P(None, ("dp", "ep"), None, None)
    return jax.shard_map(body, mesh=mesh,
                         in_specs=(spec_in, spec_in, spec_in, P(None, None)),
                         out_specs=(spec_out, spec_out), check_vma=False)
```

```python
import functools

import jax
import jax.numpy as jnp
from jax import lax
from jax.experimental import pallas as pl
from jax.experimental.pallas import tpu as pltpu
from jax.sharding import PartitionSpec as P

C = 8
NI = 3
NO = 4
NV = 3
LAG = 4
LATE = ((4, 3), (3, 0), (0, 0), (0, 0))
DIRECT = 3
DELAY1 = 2
DELAY3 = 0
FIRST_KEPT = 64
LAST = 4
BUF_P, BUF_Q, BUF_R, BUF_S = range(4)
MOVE_VMEM = 7 * 1024 * 1024
PLACE_VMEM = 7 * 1024 * 1024
STEP = 2


def _slot_of(place, a, g, j):
    return place[0, (a * 4 + g) * 2 + j] % 2


def _move(place, wg, wu, wd, st, kv0, kv1, i1, o1, i2, o2, ring, i1_sem, o1_sem, i2_sem, o2_sem, k_sem, fwd_sem, recv_sem):
    kv = (kv0, kv1)
    tiles = wg.shape[1]
    per = tiles // C
    total = 3 * per
    a = lax.axis_index("dp")
    g = lax.axis_index("ep")
    x, c = g // 2, g % 2

    def here(a2, c2):
        return (a == a2) & (c == c2)

    def dev(a2, c2):
        return (a2, 2 * x + c2)

    def within(q, fn, lo=0, hi=total):
        pl.when((q >= lo) & (q < hi))(fn)

    def local(q, fn, lo=0):
        for m, w in enumerate((wg, wu, wd)):
            within(q, lambda w=w, m=m: fn(lambda e: w.at[e, pl.ds((q - m * per) * C, C)]), jnp.maximum(lo, m * per), (m + 1) * per)

    def stage(b, q):
        return st.at[b, pl.ds(q * C, C)]

    def remote(src, dst, ssem, rsem, device):
        return pltpu.make_async_remote_copy(src_ref=src, dst_ref=dst, send_sem=ssem, recv_sem=rsem, device_id=device,
                                            device_id_type=pl.DeviceIdType.MESH)

    def wait_recv(b, q):
        within(q, lambda: remote(stage(b, q), stage(b, q), fwd_sem.at[0, 0], recv_sem.at[b, q], dev(a, 1 - c)).wait_recv())

    def forward(q, b, flow, device, hi=total):
        within(q, lambda: remote(stage(b, q), stage(b, q), fwd_sem.at[flow, q // per], recv_sem.at[b, q], device).start(), 0, hi)

    def wait_sent(flow, b, device, hi=total):
        for m in range(3):
            at = pl.ds(m * tiles, min(tiles, hi * C - m * tiles))
            remote(st.at[b, at], st.at[b, at], fwd_sem.at[flow, m], recv_sem.at[b, 0], device).wait_send()

    def pick_run(q, i, o, i_sem, o_sem, which, b, device, lo, hi):
        slot, oslot = q % NI, q % NO

        def free():
            remote(o.at[oslot], stage(b, q), o_sem.at[oslot], recv_sem.at[b, 0], device).wait_send()
        within(q, free, lo + NO, hi)

        def go():
            for e in range(2):
                pltpu.make_async_copy(st.at[0, pl.ds(0, C)], i.at[slot, e], i_sem.at[slot, e]).wait()

            def some(r, _):
                at = pl.ds(r * STEP, STEP)
                o[oslot, at] = jnp.where(which == 0, i[slot, 0, at], i[slot, 1, at])
                return 0
            lax.fori_loop(0, C // STEP, some, 0)
        within(q, go, lo, hi)

    def pick_send(q, o, o_sem, b, device, lo, hi):
        within(q, lambda: remote(o.at[q % NO], stage(b, q), o_sem.at[q % NO], recv_sem.at[b, q], device).start(), lo, hi)

    def pick_drain(o, o_sem, b, device, lo, hi):
        for n in range(NO):
            q = hi - NO + n
            within(q, lambda: remote(o.at[q % NO], stage(b, q), o_sem.at[q % NO], recv_sem.at[b, 0], device).wait_send(), lo, hi)

    mirror = (a, 2 * (1 - x) + c)
    other = 2 * (1 - x)
    far = _slot_of(place, 2, other, 1), _slot_of(place, 1, other + 1, 1)
    which = jnp.where(c == 0, far[0], far[1])
    which = jnp.where(here(1, 0) | here(2, 1), 1 - which, which)
    which = jnp.where(here(0, 1), _slot_of(place, 0, other + 1, 1), which)
    is_src = (c == 0) & (a < 2) | (c == 1) & (a >= 2)
    lo = jnp.where(is_src, 0, jnp.where(here(0, 1) | here(3, 0), total - DIRECT, total))
    delay = jnp.where(is_src, 0, jnp.where(c == 1, DELAY1, DELAY3))
    b = jnp.where(is_src, a % 2, jnp.where(c == 1, BUF_R, BUF_P))

    def pick_start(q):
        def go(src):
            for e in range(2):
                pltpu.make_async_copy(src(e), i1.at[q % NI, e], i1_sem.at[q % NI, e]).start()
        local(q, go, lo)

    def pick(q):
        pick_run(q, i1, o1, i1_sem, o1_sem, which, b, mirror, lo, total)

    far_a, far_b = _slot_of(place, 2, 2 * x, 1), _slot_of(place, 1, 2 * x + 1, 1)
    which2 = jnp.where(_slot_of(place, 0, 2 * x + 1, 1) == far_b, 1, 0)
    short = total - DIRECT

    def second(u):
        pick_send(u - 2, o2, o2_sem, BUF_R, dev(0, 1), 0, short)
        wait_recv(BUF_P, u)
        wait_recv(BUF_Q, u)
        pick_run(u - 1, i2, o2, i2_sem, o2_sem, which2, BUF_R, dev(0, 1), 0, short)

        def go():
            for e, block in enumerate((BUF_P, BUF_Q)):
                pltpu.make_async_copy(stage(block, u), i2.at[u % NI, e], i2_sem.at[u % NI, e]).start()
        within(u, go, 0, short)

    flows = {
        (0, 0): (BUF_P, ((dev(1, 0), total), (dev(2, 0), total), (dev(0, 1), total))),
        (0, 1): (BUF_Q, ((dev(0, 0), total),)),
        (1, 0): (BUF_Q, ((dev(0, 1), total), (dev(3, 0), total))),
        (2, 0): (BUF_P, ((dev(3, 0), short),)),
        (3, 1): (BUF_Q, ((dev(2, 1), total), (dev(1, 1), total))),
    }
    late = {(0, 0): (BUF_Q, BUF_R, BUF_S), (0, 1): (BUF_P, BUF_R), (1, 0): (BUF_P,), (1, 1): (BUF_Q,), (3, 0): (BUF_P, BUF_Q)}

    own = (here(1, 1) | here(2, 0) | here(3, 1), here(3, 1))
    pairs = ((jnp.where(here(0, 0), BUF_R, BUF_P), jnp.where(here(0, 0), BUF_S, BUF_Q)),
             (jnp.where(here(0, 1), BUF_R, jnp.where(here(1, 1), BUF_Q, BUF_P)),
              jnp.where(here(0, 1), BUF_R, jnp.where(here(2, 0), BUF_P, BUF_Q))))
    kept = []
    for j in range(2):
        e = _slot_of(place, a, g, j)
        from_a = (c == 0) | (here(0, 1) if j == 0 else False)
        near = own[j] | (here(0, 0) if j == 0 else False)
        kept.append(jnp.where(near, e, jnp.where(from_a, jnp.where(e == far_a, 0, 1), jnp.where(e == far_b, 1, 0))))

    def keep_to(q, j, e):
        return kv[j].at[pl.ds((q - FIRST_KEPT) * C, C)] if e == 0 else ring.at[q % NV, j]

    def keep_start(q):
        for j in range(2):
            def fetch(src, j=j):
                for e in range(2):
                    pltpu.make_async_copy(src(e), keep_to(q, j, e), k_sem.at[q % NV, j, e]).start()

            @pl.when(own[j])
            def _():
                local(jnp.where(q < total - LAST, q, -1), fetch, FIRST_KEPT)

            @pl.when(jnp.logical_not(own[j]))
            def _():
                within(q, lambda: fetch(lambda e: stage(pairs[j][e], q)), FIRST_KEPT, total - LAST)

    def keep_run(q):
        def go():
            for j in range(2):
                for e in range(2):
                    pltpu.make_async_copy(st.at[0, pl.ds(0, C)], keep_to(q, j, e), k_sem.at[q % NV, j, e]).wait()

                def some(r, _):
                    at = pl.ds((q - FIRST_KEPT) * C + r * STEP, STEP)
                    kv[j][at] = jnp.where(kept[j] == 0, kv[j][at], ring[q % NV, j, pl.ds(r * STEP, STEP)])
                    return 0
                lax.fori_loop(0, C // STEP, some, 0)
        within(q, go, FIRST_KEPT, total - LAST)

    barrier = pltpu.get_barrier_semaphore()

    def greet(*partners):
        for device in partners:
            pl.semaphore_signal(barrier, inc=1, device_id=device, device_id_type=pl.DeviceIdType.MESH)

    partners = {
        (0, 0): (mirror, dev(1, 0), dev(2, 0), dev(0, 1)),
        (0, 1): (mirror, dev(0, 0), dev(1, 0), dev(2, 1)),
        (1, 0): (mirror, dev(0, 0), dev(0, 1), dev(3, 0)),
        (1, 1): (dev(3, 1),),
        (2, 0): (dev(0, 0), dev(3, 0)),
        (2, 1): (mirror, dev(3, 1), dev(0, 1)),
        (3, 0): (mirror, dev(1, 0), dev(2, 0)),
        (3, 1): (mirror, dev(2, 1), dev(1, 1)),
    }
    for (a2, c2), devices in partners.items():
        pl.when(here(a2, c2))(functools.partial(greet, *devices))

    def early(t, _):
        pick_start(t - delay)
        return 0
    lax.fori_loop(0, 3, early, 0)
    pick(0 - delay)
    for (a2, c2), devices in partners.items():
        pl.when(here(a2, c2))(lambda devices=devices: pl.semaphore_wait(barrier, len(devices)))

    behind = jnp.int32(0)
    for a2, cores in enumerate(LATE):
        for c2, n in enumerate(cores):
            behind = jnp.where(here(a2, c2), n, behind)

    def tick(t, _):
        u = t - 3 - LAG
        pick_send(t - 3 - delay, o1, o1_sem, b, mirror, lo, total)
        pick_start(t - delay)
        pick(t - 2 - delay)

        @pl.when(here(0, 1))
        def _():
            q = t - 3

            def give(src):
                for e in range(2):
                    remote(src(e), stage(BUF_R + e, q), fwd_sem.at[1 + e, q // per], recv_sem.at[BUF_R + e, q], dev(0, 0)).start()
            local(q, give)

        @pl.when(here(2, 1))
        def _():
            second(u)

        for (a2, c2), (block, devices) in flows.items():
            @pl.when(here(a2, c2))
            def _():
                wait_recv(block, u)
                for flow, (device, hi) in enumerate(devices):
                    forward(u, block, flow, device, hi)

        v = u - behind
        for (a2, c2), blocks in late.items():
            @pl.when(here(a2, c2))
            def _():
                for block in blocks:
                    wait_recv(block, v)
        keep_start(v)
        keep_run(v - 2)
        return 0
    lax.fori_loop(3, total + 3 + LAG + max(map(max, LATE)), tick, 0)

    pick_drain(o1, o1_sem, b, mirror, lo, total)

    @pl.when(here(2, 1))
    def _():
        pick_drain(o2, o2_sem, BUF_R, dev(0, 1), 0, short)

    for (a2, c2), (block, devices) in flows.items():
        @pl.when(here(a2, c2))
        def _():
            for flow, (device, hi) in enumerate(devices):
                wait_sent(flow, block, device, hi)

    @pl.when(here(0, 1))
    def _():
        wait_sent(1, BUF_R, dev(0, 0))
        wait_sent(2, BUF_S, dev(0, 0))


T = 32
NB = 8
AHEAD = 4
PARTS = 4
SPREAD = 2


def _place(place, wg, wu, wd, st, kv0, kv1, w13, w2, buf, in_sem, out_sem, k_sem):
    kv = (kv0, kv1)
    a = lax.axis_index("dp")
    g = lax.axis_index("ep")
    x, c = g // 2, g % 2
    tiles = wg.shape[1]
    wide = w13.shape[2] // 2
    rest = FIRST_KEPT * C
    end = 3 * tiles - LAST * C
    n = rest // T
    total = 2 * (n + 1)

    far_a, far_b = _slot_of(place, 2, 2 * x, 1), _slot_of(place, 1, 2 * x + 1, 1)

    def source(j):
        e = _slot_of(place, a, g, j)
        from_a = jnp.where(e == far_a, 2 + BUF_P, 2 + BUF_Q)
        from_b = jnp.where(e == far_b, 2 + BUF_Q, 2 + BUF_P)
        if j == 0:
            c0 = jnp.where(a == 0, 2 + BUF_R + e, jnp.where(a == 2, e, from_a))
            c1 = jnp.where(a == 0, from_a, jnp.where(a == 2, from_b, e))
        else:
            c0 = jnp.where(a == 2, 2 + BUF_P, from_a)
            c1 = jnp.where(a == 0, 2 + BUF_R, jnp.where(a == 3, e, jnp.where(a == 1, 2 + BUF_Q, from_b)))
        return jnp.where(c == 0, c0, c1)

    sources = [source(0), source(1)]

    def fetch(t):
        slot = t % NB
        s = jnp.where(t % 2 == 0, sources[0], sources[1])
        k = t // 2
        low = jnp.where(k < n, k * T, end)
        m = low // tiles
        for mm, w in enumerate((wg, wu, wd)):
            @pl.when((s < 2) & (m == mm))
            def _():
                pltpu.make_async_copy(w.at[s, pl.ds(low - mm * tiles, T)], buf.at[slot], in_sem.at[slot]).start()

        @pl.when(s >= 2)
        def _():
            pltpu.make_async_copy(st.at[s - 2, pl.ds(low, T)], buf.at[slot], in_sem.at[slot]).start()

    def put(t, wait):
        k = t // 2
        m = k * T // tiles
        src, sem = buf.at[t % NB], out_sem.at[t % NB]

        @pl.when(k < n)
        def _():
            cp = pltpu.make_async_copy(src, w13.at[t % 2, pl.ds(k * T - m * tiles, T), pl.ds(m * wide, wide)], sem)
            cp.wait() if wait else cp.start()

        @pl.when(k == n)
        def _():
            cp = pltpu.make_async_copy(src, w2.at[t % 2, pl.ds(end - 2 * tiles, T)], sem)
            cp.wait() if wait else cp.start()

    def kept():
        for j in range(2):
            for m in range(2):
                low, high = max(rest, m * tiles), (m + 1) * tiles
                step = T * max(1, (high - low) // T // PARTS)
                for p, at in enumerate(range(low, high, step)):
                    size = min(step, high - at)
                    yield pltpu.make_async_copy(kv[j].at[pl.ds(at - rest, size)],
                                                w13.at[j, pl.ds(at - m * tiles, size), pl.ds(m * wide, wide)], k_sem.at[m, j, p])
            step = tiles // PARTS
            for p in range(PARTS):
                size = min(step, end - 2 * tiles - p * step)
                yield pltpu.make_async_copy(kv[j].at[pl.ds(2 * tiles - rest + p * step, size)], w2.at[j, pl.ds(p * step, size)], k_sem.at[2, j, p])

    def tick(t, _):
        @pl.when(t < total)
        def _():
            @pl.when(t >= NB)
            def _():
                put(t - NB, True)
            fetch(t)

        for n, cp in enumerate(kept()):
            pl.when(t == AHEAD - 1 + n * SPREAD)(cp.start)
        u = t - AHEAD

        @pl.when(u >= 0)
        def _():
            slot = u % NB
            pltpu.make_async_copy(st.at[0, pl.ds(0, T)], buf.at[slot], in_sem.at[slot]).wait()
            put(u, False)
        return 0
    lax.fori_loop(0, total + AHEAD, tick, 0)

    def drain(t, _):
        put(t, True)
        return 0
    lax.fori_loop(total - NB, total, drain, 0)
    for cp in kept():
        cp.wait()


def _tiles(w, wide):
    _, e, r, k = w.shape
    return w.reshape(e, r // 8, 8, k // 128, 128).transpose(0, 1, 3, 2, 4).reshape(e, -1, wide, 8, 128)


def solution(mesh):
    def body(w_gate, w_up, w_down, place):
        d, f = w_gate.shape[2], w_gate.shape[3]
        bf16 = w_gate.dtype
        wg, wu, wd = (pltpu.with_memory_space_constraint(_tiles(w, f // 128), pltpu.HBM) for w in (w_gate, w_up, w_down))
        tiles, row = wg.shape[1], wg.shape[2:]
        hbm = pl.BlockSpec(memory_space=pltpu.HBM)
        smem = pl.BlockSpec(memory_space=pltpu.SMEM)
        kept = pl.BlockSpec(memory_space=pltpu.VMEM)
        vmem, dma = pltpu.VMEM, pltpu.SemaphoreType.DMA
        shape = jax.ShapeDtypeStruct
        keep = vmem((3 * tiles - (FIRST_KEPT + LAST) * C, *row), bf16)
        st, kv0, kv1 = pl.pallas_call(
            _move,
            out_shape=(shape((4, 3 * tiles, *row), bf16), keep, keep),
            in_specs=[smem, hbm, hbm, hbm],
            out_specs=(hbm, kept, kept),
            scratch_shapes=[vmem((NI, 2, C, *row), bf16), vmem((NO, C, *row), bf16), vmem((NI, 2, C, *row), bf16),
                            vmem((NO, C, *row), bf16), vmem((NV, 2, C, *row), bf16), dma((NI, 2)), dma((NO,)), dma((NI, 2)),
                            dma((NO,)), dma((NV, 2, 2)), dma((3, 3)), dma((4, 3 * tiles // C))],
            compiler_params=pltpu.CompilerParams(collective_id=0, has_side_effects=True, vmem_limit_bytes=MOVE_VMEM),
            name="move",
        )(place, wg, wu, wd)
        w13, w2 = pl.pallas_call(
            _place,
            out_shape=(shape((2, d // 8, f // 64, 8, 128), bf16), shape((2, tiles, *row), bf16)),
            in_specs=[smem, hbm, hbm, hbm, hbm, kept, kept],
            out_specs=(hbm, hbm),
            scratch_shapes=[vmem((NB, T, *row), bf16), dma((NB,)), dma((NB,)), dma((3, 2, 2 * PARTS))],
            compiler_params=pltpu.CompilerParams(vmem_limit_bytes=PLACE_VMEM),
            name="place",
        )(place, wg, wu, wd, pltpu.with_memory_space_constraint(st, pltpu.HBM), kv0, kv1)
        w13 = w13.transpose(0, 1, 3, 2, 4).reshape(1, 2, d, 2 * f)
        w2 = w2.reshape(2, f // 8, d // 128, 8, 128).transpose(0, 1, 3, 2, 4).reshape(1, 2, f, d)
        return w13, w2

    spec_in = P(None, "ep", None, None)
    spec_out = P(None, ("dp", "ep"), None, None)
    return jax.shard_map(body, mesh=mesh,
                         in_specs=(spec_in, spec_in, spec_in, P(None, None)),
                         out_specs=(spec_out, spec_out), check_vma=False)
```

```python
import functools

import jax
import jax.numpy as jnp
from jax import lax
from jax.experimental import pallas as pl
from jax.experimental.pallas import tpu as pltpu
from jax.sharding import PartitionSpec as P

C = 8
NI = 3
NO = 4
NV = 3
LAG = 4
LATE = ((4, 3), (3, 0), (0, 0), (0, 0))
DIRECT = 3
DELAY1 = 2
DELAY3 = 0
FIRST_KEPT = 64
LAST = 4
BUF_P, BUF_Q, BUF_R, BUF_S = range(4)
MOVE_VMEM = 7 * 1024 * 1024
PLACE_VMEM = 7 * 1024 * 1024
STEP = 2


def _slot_of(place, a, g, j):
    return place[0, (a * 4 + g) * 2 + j] % 2


def _move(place, wg, wu, wd, st, kv0, kv1, i1, o1, i2, o2, ring, i1_sem, o1_sem, i2_sem, o2_sem, k_sem, fwd_sem, recv_sem):
    kv = (kv0, kv1)
    tiles = wg.shape[1]
    per = tiles // C
    total = 3 * per
    a = lax.axis_index("dp")
    g = lax.axis_index("ep")
    x, c = g // 2, g % 2

    def here(a2, c2):
        return (a == a2) & (c == c2)

    def dev(a2, c2):
        return (a2, 2 * x + c2)

    def within(q, fn, lo=0, hi=total):
        pl.when((q >= lo) & (q < hi))(fn)

    def local(q, fn, lo=0):
        for m, w in enumerate((wg, wu, wd)):
            within(q, lambda w=w, m=m: fn(lambda e: w.at[e, pl.ds((q - m * per) * C, C)]), jnp.maximum(lo, m * per), (m + 1) * per)

    def stage(b, q):
        return st.at[b, pl.ds(q * C, C)]

    def remote(src, dst, ssem, rsem, device):
        return pltpu.make_async_remote_copy(src_ref=src, dst_ref=dst, send_sem=ssem, recv_sem=rsem, device_id=device,
                                            device_id_type=pl.DeviceIdType.MESH)

    def wait_recv(b, q):
        within(q, lambda: remote(stage(b, q), stage(b, q), fwd_sem.at[0, 0], recv_sem.at[b, q], dev(a, 1 - c)).wait_recv())

    def forward(q, b, flow, device, hi=total):
        within(q, lambda: remote(stage(b, q), stage(b, q), fwd_sem.at[flow, q // per], recv_sem.at[b, q], device).start(), 0, hi)

    def wait_sent(flow, b, device, hi=total):
        for m in range(3):
            at = pl.ds(m * tiles, min(tiles, hi * C - m * tiles))
            remote(st.at[b, at], st.at[b, at], fwd_sem.at[flow, m], recv_sem.at[b, 0], device).wait_send()

    def pick_run(q, i, o, i_sem, o_sem, which, b, device, lo, hi):
        slot, oslot = q % NI, q % NO

        def free():
            remote(o.at[oslot], stage(b, q), o_sem.at[oslot], recv_sem.at[b, 0], device).wait_send()
        within(q, free, lo + NO, hi)

        def go():
            for e in range(2):
                pltpu.make_async_copy(st.at[0, pl.ds(0, C)], i.at[slot, e], i_sem.at[slot, e]).wait()

            def some(r, _):
                at = pl.ds(r * STEP, STEP)
                o[oslot, at] = jnp.where(which == 0, i[slot, 0, at], i[slot, 1, at])
                return 0
            lax.fori_loop(0, C // STEP, some, 0)
        within(q, go, lo, hi)

    def pick_send(q, o, o_sem, b, device, lo, hi):
        within(q, lambda: remote(o.at[q % NO], stage(b, q), o_sem.at[q % NO], recv_sem.at[b, q], device).start(), lo, hi)

    def pick_drain(o, o_sem, b, device, lo, hi):
        for n in range(NO):
            q = hi - NO + n
            within(q, lambda: remote(o.at[q % NO], stage(b, q), o_sem.at[q % NO], recv_sem.at[b, 0], device).wait_send(), lo, hi)

    mirror = (a, 2 * (1 - x) + c)
    other = 2 * (1 - x)
    far = _slot_of(place, 2, other, 1), _slot_of(place, 1, other + 1, 1)
    which = jnp.where(c == 0, far[0], far[1])
    which = jnp.where(here(1, 0) | here(2, 1), 1 - which, which)
    which = jnp.where(here(0, 1), _slot_of(place, 0, other + 1, 1), which)
    is_src = (c == 0) & (a < 2) | (c == 1) & (a >= 2)
    lo = jnp.where(is_src, 0, jnp.where(here(0, 1) | here(3, 0), total - DIRECT, total))
    delay = jnp.where(is_src, 0, jnp.where(c == 1, DELAY1, DELAY3))
    b = jnp.where(is_src, a % 2, jnp.where(c == 1, BUF_R, BUF_P))

    def pick_start(q):
        def go(src):
            for e in range(2):
                pltpu.make_async_copy(src(e), i1.at[q % NI, e], i1_sem.at[q % NI, e]).start()
        local(q, go, lo)

    def pick(q):
        pick_run(q, i1, o1, i1_sem, o1_sem, which, b, mirror, lo, total)

    far_a, far_b = _slot_of(place, 2, 2 * x, 1), _slot_of(place, 1, 2 * x + 1, 1)
    which2 = jnp.where(_slot_of(place, 0, 2 * x + 1, 1) == far_b, 1, 0)
    short = total - DIRECT

    def second(u):
        pick_send(u - 2, o2, o2_sem, BUF_R, dev(0, 1), 0, short)
        wait_recv(BUF_P, u)
        wait_recv(BUF_Q, u)
        pick_run(u - 1, i2, o2, i2_sem, o2_sem, which2, BUF_R, dev(0, 1), 0, short)

        def go():
            for e, block in enumerate((BUF_P, BUF_Q)):
                pltpu.make_async_copy(stage(block, u), i2.at[u % NI, e], i2_sem.at[u % NI, e]).start()
        within(u, go, 0, short)

    flows = {
        (0, 0): (BUF_P, ((dev(1, 0), total), (dev(2, 0), total), (dev(0, 1), total))),
        (0, 1): (BUF_Q, ((dev(0, 0), total),)),
        (1, 0): (BUF_Q, ((dev(0, 1), total), (dev(3, 0), total))),
        (2, 0): (BUF_P, ((dev(3, 0), short),)),
        (3, 1): (BUF_Q, ((dev(2, 1), total), (dev(1, 1), total))),
    }
    late = {(0, 0): (BUF_Q, BUF_R, BUF_S), (0, 1): (BUF_P, BUF_R), (1, 0): (BUF_P,), (1, 1): (BUF_Q,), (3, 0): (BUF_P, BUF_Q)}

    own = (here(1, 1) | here(2, 0) | here(3, 1), here(3, 1))
    pairs = ((jnp.where(here(0, 0), BUF_R, BUF_P), jnp.where(here(0, 0), BUF_S, BUF_Q)),
             (jnp.where(here(0, 1), BUF_R, jnp.where(here(1, 1), BUF_Q, BUF_P)),
              jnp.where(here(0, 1), BUF_R, jnp.where(here(2, 0), BUF_P, BUF_Q))))
    kept = []
    for j in range(2):
        e = _slot_of(place, a, g, j)
        from_a = (c == 0) | (here(0, 1) if j == 0 else False)
        near = own[j] | (here(0, 0) if j == 0 else False)
        kept.append(jnp.where(near, e, jnp.where(from_a, jnp.where(e == far_a, 0, 1), jnp.where(e == far_b, 1, 0))))

    def keep_to(q, j, e):
        return kv[j].at[pl.ds((q - FIRST_KEPT) * C, C)] if e == 0 else ring.at[q % NV, j]

    def keep_start(q):
        for j in range(2):
            def fetch(src, j=j):
                for e in range(2):
                    pltpu.make_async_copy(src(e), keep_to(q, j, e), k_sem.at[q % NV, j, e]).start()

            @pl.when(own[j])
            def _():
                local(jnp.where(q < total - LAST, q, -1), fetch, FIRST_KEPT)

            @pl.when(jnp.logical_not(own[j]))
            def _():
                within(q, lambda: fetch(lambda e: stage(pairs[j][e], q)), FIRST_KEPT, total - LAST)

    def keep_run(q):
        def go():
            for j in range(2):
                for e in range(2):
                    pltpu.make_async_copy(st.at[0, pl.ds(0, C)], keep_to(q, j, e), k_sem.at[q % NV, j, e]).wait()

                def some(r, _):
                    at = pl.ds((q - FIRST_KEPT) * C + r * STEP, STEP)
                    kv[j][at] = jnp.where(kept[j] == 0, kv[j][at], ring[q % NV, j, pl.ds(r * STEP, STEP)])
                    return 0
                lax.fori_loop(0, C // STEP, some, 0)
        within(q, go, FIRST_KEPT, total - LAST)

    barrier = pltpu.get_barrier_semaphore()

    def greet(*partners):
        for device in partners:
            pl.semaphore_signal(barrier, inc=1, device_id=device, device_id_type=pl.DeviceIdType.MESH)

    partners = {
        (0, 0): (mirror, dev(1, 0), dev(2, 0), dev(0, 1)),
        (0, 1): (mirror, dev(0, 0), dev(1, 0), dev(2, 1)),
        (1, 0): (mirror, dev(0, 0), dev(0, 1), dev(3, 0)),
        (1, 1): (dev(3, 1),),
        (2, 0): (dev(0, 0), dev(3, 0)),
        (2, 1): (mirror, dev(3, 1), dev(0, 1)),
        (3, 0): (mirror, dev(1, 0), dev(2, 0)),
        (3, 1): (mirror, dev(2, 1), dev(1, 1)),
    }
    for (a2, c2), devices in partners.items():
        pl.when(here(a2, c2))(functools.partial(greet, *devices))

    def early(t, _):
        pick_start(t - delay)
        return 0
    lax.fori_loop(0, 3, early, 0)
    pick(0 - delay)
    for (a2, c2), devices in partners.items():
        pl.when(here(a2, c2))(lambda devices=devices: pl.semaphore_wait(barrier, len(devices)))

    behind = jnp.int32(0)
    for a2, cores in enumerate(LATE):
        for c2, n in enumerate(cores):
            behind = jnp.where(here(a2, c2), n, behind)

    def tick(t, _):
        u = t - 3 - LAG
        pick_send(t - 3 - delay, o1, o1_sem, b, mirror, lo, total)
        pick_start(t - delay)
        pick(t - 2 - delay)

        @pl.when(here(0, 1))
        def _():
            q = t - 3

            def give(src):
                for e in range(2):
                    remote(src(e), stage(BUF_R + e, q), fwd_sem.at[1 + e, q // per], recv_sem.at[BUF_R + e, q], dev(0, 0)).start()
            local(q, give)

        @pl.when(here(2, 1))
        def _():
            second(u)

        for (a2, c2), (block, devices) in flows.items():
            @pl.when(here(a2, c2))
            def _():
                wait_recv(block, u)
                for flow, (device, hi) in enumerate(devices):
                    forward(u, block, flow, device, hi)

        v = u - behind
        for (a2, c2), blocks in late.items():
            @pl.when(here(a2, c2))
            def _():
                for block in blocks:
                    wait_recv(block, v)
        keep_start(v)
        keep_run(v - 2)
        return 0
    lax.fori_loop(3, total + 3 + LAG + max(map(max, LATE)), tick, 0)

    pick_drain(o1, o1_sem, b, mirror, lo, total)

    @pl.when(here(2, 1))
    def _():
        pick_drain(o2, o2_sem, BUF_R, dev(0, 1), 0, short)

    for (a2, c2), (block, devices) in flows.items():
        @pl.when(here(a2, c2))
        def _():
            for flow, (device, hi) in enumerate(devices):
                wait_sent(flow, block, device, hi)

    @pl.when(here(0, 1))
    def _():
        wait_sent(1, BUF_R, dev(0, 0))
        wait_sent(2, BUF_S, dev(0, 0))


T = 32
NB = 8
AHEAD = 4
PARTS = 4
SPREAD = 2


def _place(place, wg, wu, wd, st, kv0, kv1, w13, w2, buf, in_sem, out_sem, k_sem):
    kv = (kv0, kv1)
    a = lax.axis_index("dp")
    g = lax.axis_index("ep")
    x, c = g // 2, g % 2
    tiles = wg.shape[1]
    wide = w13.shape[2] // 2
    rest = FIRST_KEPT * C
    end = 3 * tiles - LAST * C
    n = rest // T
    total = 2 * (n + 1)

    far_a, far_b = _slot_of(place, 2, 2 * x, 1), _slot_of(place, 1, 2 * x + 1, 1)

    def source(j):
        e = _slot_of(place, a, g, j)
        from_a = jnp.where(e == far_a, 2 + BUF_P, 2 + BUF_Q)
        from_b = jnp.where(e == far_b, 2 + BUF_Q, 2 + BUF_P)
        if j == 0:
            c0 = jnp.where(a == 0, 2 + BUF_R + e, jnp.where(a == 2, e, from_a))
            c1 = jnp.where(a == 0, from_a, jnp.where(a == 2, from_b, e))
        else:
            c0 = jnp.where(a == 2, 2 + BUF_P, from_a)
            c1 = jnp.where(a == 0, 2 + BUF_R, jnp.where(a == 3, e, jnp.where(a == 1, 2 + BUF_Q, from_b)))
        return jnp.where(c == 0, c0, c1)

    sources = [source(0), source(1)]

    def fetch(t):
        slot = t % NB
        s = jnp.where(t % 2 == 0, sources[0], sources[1])
        k = t // 2
        low = jnp.where(k < n, k * T, end)
        m = low // tiles
        for mm, w in enumerate((wg, wu, wd)):
            @pl.when((s < 2) & (m == mm))
            def _():
                pltpu.make_async_copy(w.at[s, pl.ds(low - mm * tiles, T)], buf.at[slot], in_sem.at[slot]).start()

        @pl.when(s >= 2)
        def _():
            pltpu.make_async_copy(st.at[s - 2, pl.ds(low, T)], buf.at[slot], in_sem.at[slot]).start()

    def put(t, wait):
        k = t // 2
        m = k * T // tiles
        src, sem = buf.at[t % NB], out_sem.at[t % NB]

        @pl.when(k < n)
        def _():
            cp = pltpu.make_async_copy(src, w13.at[t % 2, pl.ds(k * T - m * tiles, T), pl.ds(m * wide, wide)], sem)
            cp.wait() if wait else cp.start()

        @pl.when(k == n)
        def _():
            cp = pltpu.make_async_copy(src, w2.at[t % 2, pl.ds(end - 2 * tiles, T)], sem)
            cp.wait() if wait else cp.start()

    def kept():
        for j in range(2):
            for m in range(2):
                low, high = max(rest, m * tiles), (m + 1) * tiles
                step = T * max(1, (high - low) // T // PARTS)
                for p, at in enumerate(range(low, high, step)):
                    size = min(step, high - at)
                    yield pltpu.make_async_copy(kv[j].at[pl.ds(at - rest, size)],
                                                w13.at[j, pl.ds(at - m * tiles, size), pl.ds(m * wide, wide)], k_sem.at[m, j, p])
            step = tiles // PARTS
            for p in range(PARTS):
                size = min(step, end - 2 * tiles - p * step)
                yield pltpu.make_async_copy(kv[j].at[pl.ds(2 * tiles - rest + p * step, size)], w2.at[j, pl.ds(p * step, size)], k_sem.at[2, j, p])

    def tick(t, _):
        @pl.when(t < total)
        def _():
            @pl.when(t >= NB)
            def _():
                put(t - NB, True)
            fetch(t)

        for n, cp in enumerate(kept()):
            pl.when(t == AHEAD - 1 + n * SPREAD)(functools.partial(cp.start, priority=1))
        u = t - AHEAD

        @pl.when(u >= 0)
        def _():
            slot = u % NB
            pltpu.make_async_copy(st.at[0, pl.ds(0, T)], buf.at[slot], in_sem.at[slot]).wait()
            put(u, False)
        return 0
    lax.fori_loop(0, total + AHEAD, tick, 0)

    def drain(t, _):
        put(t, True)
        return 0
    lax.fori_loop(total - NB, total, drain, 0)
    for cp in kept():
        cp.wait()


def _tiles(w, wide):
    _, e, r, k = w.shape
    return w.reshape(e, r // 8, 8, k // 128, 128).transpose(0, 1, 3, 2, 4).reshape(e, -1, wide, 8, 128)


def solution(mesh):
    def body(w_gate, w_up, w_down, place):
        d, f = w_gate.shape[2], w_gate.shape[3]
        bf16 = w_gate.dtype
        wg, wu, wd = (pltpu.with_memory_space_constraint(_tiles(w, f // 128), pltpu.HBM) for w in (w_gate, w_up, w_down))
        tiles, row = wg.shape[1], wg.shape[2:]
        hbm = pl.BlockSpec(memory_space=pltpu.HBM)
        smem = pl.BlockSpec(memory_space=pltpu.SMEM)
        kept = pl.BlockSpec(memory_space=pltpu.VMEM)
        vmem, dma = pltpu.VMEM, pltpu.SemaphoreType.DMA
        shape = jax.ShapeDtypeStruct
        keep = vmem((3 * tiles - (FIRST_KEPT + LAST) * C, *row), bf16)
        st, kv0, kv1 = pl.pallas_call(
            _move,
            out_shape=(shape((4, 3 * tiles, *row), bf16), keep, keep),
            in_specs=[smem, hbm, hbm, hbm],
            out_specs=(hbm, kept, kept),
            scratch_shapes=[vmem((NI, 2, C, *row), bf16), vmem((NO, C, *row), bf16), vmem((NI, 2, C, *row), bf16),
                            vmem((NO, C, *row), bf16), vmem((NV, 2, C, *row), bf16), dma((NI, 2)), dma((NO,)), dma((NI, 2)),
                            dma((NO,)), dma((NV, 2, 2)), dma((3, 3)), dma((4, 3 * tiles // C))],
            compiler_params=pltpu.CompilerParams(collective_id=0, has_side_effects=True, vmem_limit_bytes=MOVE_VMEM),
            name="move",
        )(place, wg, wu, wd)
        w13, w2 = pl.pallas_call(
            _place,
            out_shape=(shape((2, d // 8, f // 64, 8, 128), bf16), shape((2, tiles, *row), bf16)),
            in_specs=[smem, hbm, hbm, hbm, hbm, kept, kept],
            out_specs=(hbm, hbm),
            scratch_shapes=[vmem((NB, T, *row), bf16), dma((NB,)), dma((NB,)), dma((3, 2, 2 * PARTS))],
            compiler_params=pltpu.CompilerParams(vmem_limit_bytes=PLACE_VMEM),
            name="place",
        )(place, wg, wu, wd, pltpu.with_memory_space_constraint(st, pltpu.HBM), kv0, kv1)
        w13 = w13.transpose(0, 1, 3, 2, 4).reshape(1, 2, d, 2 * f)
        w2 = w2.reshape(2, f // 8, d // 128, 8, 128).transpose(0, 1, 3, 2, 4).reshape(1, 2, f, d)
        return w13, w2

    spec_in = P(None, "ep", None, None)
    spec_out = P(None, ("dp", "ep"), None, None)
    return jax.shard_map(body, mesh=mesh,
                         in_specs=(spec_in, spec_in, spec_in, P(None, None)),
                         out_specs=(spec_out, spec_out), check_vma=False)
```
